128 devices in a mesh: dp: 1, cp: 128 (over z, y, x, core).
Axes of the slice: x: 4, y: 4, z: 4, core: 2. Of those that a mesh axis runs over, the one named last changes fastest.
Arguments:
- queries: bfloat16 [3072, 28, 128], P(('dp', 'cp'))
- key_new: bfloat16 [3072, 4, 128], P(('dp', 'cp'))
- value_new: bfloat16 [3072, 4, 128], P(('dp', 'cp'))
- key_cache: bfloat16 [196608, 4, 128], P(('dp', 'cp'))
- value_cache: bfloat16 [196608, 4, 128], P(('dp', 'cp'))
- prefix_len: int32 [1], P('dp')
Outputs:
- output 1: bfloat16 [3072, 28, 128], P(('dp', 'cp'))
- output 2: float32 [3072, 28], P(('dp', 'cp'))
All inputs are finite; a program needn't handle non-finite values.
Results may differ from the reference program's by a relative error of at most 0.00749064.
Values are sent between devices in bfloat16 or wider.
A program may use at most 1 GiB of HBM per device.

```python
import math
import jax
import jax.numpy as jnp
from jax import lax

GROUP_SIZE = 128
NEW_DEV = 24
PREFIX_DEV = 1536
Q_HEADS = 28
KV_HEADS = 4
HEAD_DIM = 128
NEW_LEN = GROUP_SIZE * NEW_DEV
P_MAX = GROUP_SIZE * PREFIX_DEV
GROUP_RATIO = Q_HEADS // KV_HEADS


def setup_inputs(seed: int = 0, part: int = 0) -> dict:
    base_key = jax.random.fold_in(jax.random.key(seed), part)
    rand_keys = jax.random.split(base_key, 9)
    shift_scale = GROUP_SIZE ** 0.5
    new_boost = math.log(P_MAX / NEW_LEN) * 2.0 ** 0.5
    direction = jax.random.normal(rand_keys[0], (KV_HEADS, HEAD_DIM), jnp.float32)
    direction = direction / jnp.linalg.norm(direction, axis=-1, keepdims=True)
    q_mean = jnp.repeat(direction, GROUP_RATIO, axis=0) * HEAD_DIM ** 0.5
    q_noise = jax.random.normal(rand_keys[1], (NEW_LEN, Q_HEADS, HEAD_DIM), jnp.float32)
    queries = (q_noise + q_mean[None]) * 0.5 ** 0.5
    key_new = jax.random.normal(rand_keys[2], (NEW_LEN, KV_HEADS, HEAD_DIM), jnp.float32) + new_boost * direction[None]
    new_shift = jax.random.normal(rand_keys[3], (GROUP_SIZE, 1, KV_HEADS, HEAD_DIM), jnp.float32) * shift_scale
    value_new = jax.random.normal(rand_keys[4], (GROUP_SIZE, NEW_DEV, KV_HEADS, HEAD_DIM), jnp.float32) + new_shift
    key_cache = jax.random.normal(rand_keys[5], (P_MAX, KV_HEADS, HEAD_DIM), jnp.float32)
    cache_shift = jax.random.normal(rand_keys[6], (GROUP_SIZE, 1, KV_HEADS, HEAD_DIM), jnp.float32) * shift_scale
    value_cache = jax.random.normal(rand_keys[7], (GROUP_SIZE, PREFIX_DEV, KV_HEADS, HEAD_DIM), jnp.float32) + cache_shift
    prefix_len = jax.random.randint(rand_keys[8], (1,), (3 * P_MAX) // 4, P_MAX + 1, jnp.int32)
    return {
        'queries': queries.astype(jnp.bfloat16),
        'key_new': key_new.astype(jnp.bfloat16),
        'value_new': value_new.reshape(NEW_LEN, KV_HEADS, HEAD_DIM).astype(jnp.bfloat16),
        'key_cache': key_cache.astype(jnp.bfloat16),
        'value_cache': value_cache.reshape(P_MAX, KV_HEADS, HEAD_DIM).astype(jnp.bfloat16),
        'prefix_len': prefix_len,
    }


def reference(queries, key_new, value_new, key_cache, value_cache, prefix_len):
    prefix_end = prefix_len[0]
    key_pos = jnp.arange(P_MAX + NEW_LEN)
    logit_scale = HEAD_DIM ** -0.5

    def one_head(head_idx):
        kv_idx = head_idx // GROUP_RATIO
        keys_all = jnp.concatenate([lax.dynamic_index_in_dim(key_cache, kv_idx, axis=1, keepdims=False), lax.dynamic_index_in_dim(key_new, kv_idx, axis=1, keepdims=False)], axis=0).astype(jnp.float32)
        vals_all = jnp.concatenate([lax.dynamic_index_in_dim(value_cache, kv_idx, axis=1, keepdims=False), lax.dynamic_index_in_dim(value_new, kv_idx, axis=1, keepdims=False)], axis=0).astype(jnp.float32)
        q_head = lax.dynamic_index_in_dim(queries, head_idx, axis=1, keepdims=False).astype(jnp.float32).reshape(GROUP_SIZE, NEW_DEV, HEAD_DIM)

        def one_block(block_args):
            q_rows, row_start = block_args
            scores = jnp.dot(q_rows, keys_all.T) * logit_scale
            q_pos = row_start + jnp.arange(NEW_DEV)
            visible = jnp.where(key_pos[None, :] < P_MAX, key_pos[None, :] < prefix_end, key_pos[None, :] - P_MAX <= q_pos[:, None])
            scores = jnp.where(visible, scores, -jnp.inf)
            row_max = jnp.max(scores, axis=-1)
            exp_scores = jnp.exp(scores - row_max[:, None])
            row_sum = jnp.sum(exp_scores, axis=-1)
            prob_bf = exp_scores.astype(jnp.bfloat16).astype(jnp.float32)
            block_out = jnp.dot(prob_bf, vals_all) / row_sum[:, None]
            return block_out.astype(jnp.bfloat16), row_max + jnp.log(row_sum)

        head_out, head_lse = lax.map(one_block, (q_head, jnp.arange(GROUP_SIZE) * NEW_DEV))
        return head_out.reshape(NEW_LEN, HEAD_DIM), head_lse.reshape(NEW_LEN)

    all_out, all_lse = lax.map(one_head, jnp.arange(Q_HEADS))
    return jnp.transpose(all_out, (1, 0, 2)), jnp.transpose(all_lse)
```

```python
import functools
import math

import jax
import jax.numpy as jnp
from jax import lax
from jax.experimental import pallas as pl
from jax.experimental.pallas import tpu as pltpu
from jax.sharding import PartitionSpec as P

ZD, YD, XD = 4, 4, 4
SIM = True

HEADS, KV, HD = 28, 4, 128
RATIO = HEADS // KV
FILL = -1e30
SCALE2 = HD ** -0.5 * math.log2(math.e)
LN2 = math.log(2.0)
PAD = 32
BF, F32 = jnp.bfloat16, jnp.float32


def ring_offsets():
    def hops(d, n):
        return min(d, n - d)

    offs = [(dy, dz) for dz in range(ZD) for dy in range(YD)]
    return sorted(offs, key=lambda o: (hops(o[0], YD) + hops(o[1], ZD), o[1], o[0]))


class Mxu:
    def __init__(self, accs):
        self.acc = accs
        self.staged = [[None, None], [None, None]]
        self.loaded = [None, None]
        self.val = [[None] * 4, [None] * 4]

    def push(self, rhs, reg, t):
        if not SIM:
            pltpu.matmul_push_rhs(rhs, reg, t)
        else:
            self.staged[t][reg] = rhs

    def mul(self, t, a, lhs, reg):
        if not SIM:
            pltpu.matmul_acc_lhs(self.acc[t][a], lhs, load_staged_rhs=reg)
        else:
            r = jnp.dot(lhs, self.staged[t][reg], preferred_element_type=F32)
            self.val[t][a] = r if self.val[t][a] is None else self.val[t][a] + r

    def pop(self, t, a):
        if not SIM:
            return pltpu.matmul_pop(self.acc[t][a])
        r, self.val[t][a] = self.val[t][a], None
        return r


def make_kernel(tok, cache):
    offs = ring_offsets()
    G = len(offs)
    PIECE = RATIO * tok
    UNIT = XD * PIECE
    ROWS = G * UNIT
    NPAIR = -(-ROWS // 512)
    CHB = 2 * cache // 256
    NCB = XD * CHB
    NKB = NCB + 1
    LSE_ROWS = UNIT // 128 + 1
    assert cache % 256 == 0 and 8 * PAD == 256 and tok <= PAD

    def kernel(plen, q_in, k_in, v_in, n_in, tq_in, out, lse_out,
               kb, vb, bias, qx, qall, qt, sb, oacc, mb, lb, mcur, tq, keyid, nrecv,
               obuf, lbuf, orecv, lrecv, fo, fl,
               lsem, q_ss, q_rs, b_ss, b_rs, k_ss, k_rs, f_ss, n_ss, n_rs,
               o_ss, o_rs, l_ss, l_rs, x_ss, x_rs, y_ss, y_rs):
        cp = lax.axis_index("cp")
        c = cp % 2
        x = (cp // 2) % XD
        y = (cp // (2 * XD)) % YD
        z = cp // (2 * XD * YD)
        row0 = (z * YD + y) * XD

        def at(xx, yy, zz, cc):
            return ((zz * YD + yy) * XD + xx) * 2 + cc

        def x_peer(dd):
            return at((x + dd) % XD, y, z, c)

        mate = at(x, y, z, 1 - c)

        def to_peer(w):
            dy, dz = offs[w]
            return at(x, (y + dy) % YD, (z + dz) % ZD, c)

        def from_peer(w):
            dy, dz = offs[w]
            return at(x, (y + YD - dy) % YD, (z + ZD - dz) % ZD, c)

        def rc(src, dst, ss, rs, dev):
            return pltpu.make_async_remote_copy(
                src_ref=src, dst_ref=dst, send_sem=ss, recv_sem=rs,
                device_id={"cp": dev}, device_id_type=pl.DeviceIdType.MESH)

        row_devs = [(dd, dc) for dd in range(XD) for dc in range(2) if (dd, dc) != (0, 0)]

        def row_peer(dd, dc):
            return at((x + dd) % XD, y, z, (c + dc) % 2)

        barrier = pltpu.get_barrier_semaphore()
        peers = [to_peer(w) for w in range(1, G)] + [row_peer(dd, dc) for dd, dc in row_devs]
        for p in peers:
            pl.semaphore_signal(barrier, inc=1, device_id={"cp": p}, device_id_type=pl.DeviceIdType.MESH)
        me_j = x * 2 + c
        local = [
            pltpu.make_async_copy(q_in.at[x], qx.at[x], lsem.at[0]),
            pltpu.make_async_copy(k_in.at[x], kb.at[pl.ds(c * cache, cache)], lsem.at[1]),
            pltpu.make_async_copy(v_in.at[x], vb.at[pl.ds(c * cache, cache)], lsem.at[2]),
            pltpu.make_async_copy(n_in.at[x], nrecv.at[me_j], lsem.at[3]),
            pltpu.make_async_copy(tq_in, tq, lsem.at[4]),
        ]
        for cpy in local:
            cpy.start()

        prefix = plen[0]
        riota = lax.broadcasted_iota(jnp.int32, (256, 128), 0)
        lane0 = lax.broadcasted_iota(jnp.int32, (256, 128), 1) == 0
        nblk = cache // 256

        def bias_block(b, _):
            slot = b // nblk
            base = ((row0 + (x + slot // 2) % XD) * 2 + slot % 2) * cache + (b % nblk) * 256
            hide = jnp.where(lane0 & (riota + base >= prefix), FILL, 0.0)
            bias[pl.ds(pl.multiple_of(b * 256, 256), 256), :] = hide.astype(BF)
            return 0

        lax.fori_loop(0, NCB, bias_block, 0)
        bias[pl.ds(NCB * 256, 256), :] = jnp.zeros((256, 128), BF)
        dev_j = lax.shift_right_logical(riota, 5)
        r_j = lax.bitwise_and(riota, PAD - 1)
        keyid[...] = jnp.where(r_j < tok, (row0 * 2 + dev_j) * tok + r_j, 1 << 23).astype(F32)

        pl.semaphore_wait(barrier, len(peers))

        q_send = [rc(q_in.at[(x + dd) % XD], qx.at[x], q_ss.at[dd], q_rs.at[x], x_peer(dd)) for dd in range(1, XD)]
        for cpy in q_send:
            cpy.start()
        own = pl.ds(c * cache, cache)
        kv_send = [rc(k_in.at[x], kb.at[own], k_ss.at[0, 0], k_rs.at[c, 0], mate),
                   rc(v_in.at[x], vb.at[own], k_ss.at[0, 1], k_rs.at[c, 1], mate)]
        order = [1, XD - 1] + [d for d in range(2, XD - 1)]
        for dd in order:
            slot = ((XD - dd) % XD) * 2 + c
            there = pl.ds(slot * cache, cache)
            kv_send.append(rc(k_in.at[(x + dd) % XD], kb.at[there], k_ss.at[dd, 0], k_rs.at[slot, 0], x_peer(dd)))
            kv_send.append(rc(v_in.at[(x + dd) % XD], vb.at[there], k_ss.at[dd, 1], k_rs.at[slot, 1], x_peer(dd)))
        for cpy in kv_send:
            cpy.start()
        n_send = [rc(n_in.at[(x + dd) % XD], nrecv.at[me_j], n_ss.at[i], n_rs.at[me_j], row_peer(dd, dc))
                  for i, (dd, dc) in enumerate(row_devs)]
        for cpy in n_send:
            cpy.start()

        local[0].wait()
        for dd in range(1, XD):
            src = (x + dd) % XD
            rc(q_in.at[x], qx.at[src], q_ss.at[dd], q_rs.at[src], x_peer(dd)).wait_recv()
        own_rows = jnp.concatenate([qx[i].astype(F32) for i in range(XD)], axis=0).astype(BF)
        qall[pl.ds(0, UNIT), :] = own_rows
        b_send = [rc(qall.at[pl.ds(0, UNIT)], qall.at[pl.ds(w * UNIT, UNIT)], b_ss.at[w], b_rs.at[w], from_peer(w))
                  for w in range(1, G)]
        for cpy in b_send:
            cpy.start()

        def wait_unit(w):
            there = pl.ds(pl.multiple_of(w * UNIT, 16), UNIT)
            rc(qall.at[pl.ds(0, UNIT)], qall.at[there], b_ss.at[w], b_rs.at[w], mate).wait_recv()

        def units_for(p):
            return jnp.minimum((p * 512 + 511) // UNIT + 1, G)

        def prep(p):
            for t in range(2):
                rows = qall[pl.ds(pl.multiple_of((p * 2 + t) * 256, 256), 256), :]
                qt[p * 2 + t] = rows.T

        ones_row = jnp.where(lax.broadcasted_iota(jnp.int32, (128, 256), 0) == 0, 1.0, 0.0).astype(BF)

        def rep(v, n):
            return jnp.concatenate([v] * n, axis=0)

        def unit_body(mx, blocks, pv, qk, first, prep_pair):
            if prep_pair is not None:
                prep(prep_pair)
            n = len(blocks)
            if pv is not None:
                mp = [mcur[t] for t in range(2)]
                lacc = [jnp.zeros((8, 256), F32) for _ in range(2)]
            if qk is not None:
                mxs = [jnp.full((8, 256), -jnp.inf, F32) for _ in range(2)]

                def qpush(t):
                    mx.push(jnp.concatenate([qt[qk * 2 + t], ones_row], axis=0), 0, t)

                for t in range(2):
                    qpush(t)
            for i, b in enumerate(blocks):
                if qk is not None:
                    k = jnp.concatenate([kb[pl.ds(b * 256, 256), :], bias[pl.ds(b * 256, 256), :]], axis=1)
                    for t in range(2):
                        mx.mul(t, i % 3, k, 0)
                if pv is not None:
                    for t in range(2):
                        p = jnp.exp2((sb[t, i] - rep(mp[t], 32)) * SCALE2)
                        lacc[t] = lacc[t] + p.reshape(32, 8, 256).sum(0)
                        mx.push(p.astype(BF), 1, t)
                    vt = jnp.concatenate([vb[pl.ds(b * 256, 128), :], vb[pl.ds(b * 256 + 128, 128), :]], axis=1)
                    for t in range(2):
                        mx.mul(t, 3, vt, 1)
                if qk is not None:
                    if i < n - 1:
                        for t in range(2):
                            qpush(t)
                    for t in range(2):
                        s = mx.pop(t, i % 3)
                        if b == NCB:
                            lim = rep(tq[qk * 2 + t], 32)
                            kid = jnp.concatenate([keyid[...], keyid[...]], axis=1)
                            s = jnp.where(kid <= lim, s, FILL)
                        sb[t, i] = s
                        mxs[t] = jnp.maximum(mxs[t], s.reshape(32, 8, 256).max(0))
            if pv is not None:
                for t in range(2):
                    o = mx.pop(t, 3)
                    tile = pv * 2 + t
                    if first:
                        oacc[tile] = o
                        lb[tile] = lacc[t]
                    else:
                        alpha = jnp.exp2((mb[tile] - mp[t]) * SCALE2)
                        l = jnp.sum(lacc[t] + alpha * lb[tile], axis=0, keepdims=True)
                        inv = 1.0 / l
                        o = (oacc[tile] * rep(alpha, 16) + o) * inv
                        obuf[pl.ds(pl.multiple_of(tile * 256, 256), 256), :] = o.T.astype(BF)
                        ls = mp[t][0:1] * SCALE2 + jnp.log2(l)
                        lbuf[tile * 2] = ls[:, 0:128]
                        lbuf[tile * 2 + 1] = ls[:, 128:256]
            if qk is not None:
                for t in range(2):
                    m = jnp.broadcast_to(jnp.max(mxs[t], axis=0, keepdims=True), (8, 256))
                    if first:
                        mb[qk * 2 + t] = m
                    else:
                        m = jnp.maximum(m, mb[qk * 2 + t])
                    mcur[t] = m

        def compute(*accs):
            mx = Mxu([accs[:4], accs[4:]])

            for cpy in local[1:]:
                cpy.wait()
            other = pl.ds((1 - c) * cache, cache)
            rc(k_in.at[x], kb.at[other], k_ss.at[0, 0], k_rs.at[1 - c, 0], mate).wait_recv()
            rc(v_in.at[x], vb.at[other], k_ss.at[0, 1], k_rs.at[1 - c, 1], mate).wait_recv()
            u_first = int(units_for_py(min(1, NPAIR - 1)))
            for w in range(1, u_first):
                wait_unit(w)
            blocks = list(range(CHB))
            prep(0)
            unit_body(mx, blocks, None, 0, True, 1 if NPAIR > 1 else None)

            def forward(dxs):
                for dx in dxs:
                    mine = pl.ds((dx * 2 + c) * cache, cache)
                    for kv, buf in enumerate((kb, vb)):
                        rc(buf.at[mine], buf.at[mine], f_ss.at[dx, kv], k_rs.at[dx * 2 + c, kv], mate).wait_recv()
                        rc(buf.at[mine], buf.at[mine], f_ss.at[dx, kv], k_rs.at[dx * 2 + c, kv], mate).start()

            near = sorted({1, XD - 1})
            far = [d for d in range(1, XD) if d not in near]
            u_near = min(15, max(NPAIR - 3, 0))

            def pass_a(u, _):
                have, need = units_for(u + 1), units_for(u + 2)

                @pl.when(need > have)
                def _():
                    wait_unit(have)

                @pl.when(u == u_near)
                def _():
                    forward(near)

                unit_body(mx, blocks, u, u + 1, True, jnp.minimum(u + 2, NPAIR - 1))
                return 0

            lax.fori_loop(0, NPAIR - 1, pass_a, 0)
            unit_body(mx, blocks, NPAIR - 1, None, True, None)

            forward(far)
            for i in range(1, 8):
                j = (me_j + i) % 8
                rc(n_in.at[x], nrecv.at[j], n_ss.at[0], n_rs.at[j], mate).wait_recv()
            newk = jnp.concatenate([nrecv[j, 0] for j in range(8)], axis=0)
            newv = jnp.concatenate([nrecv[j, 1] for j in range(8)], axis=0).T
            kb[pl.ds(NCB * 256, 256), :] = newk
            vb[pl.ds(NCB * 256, 128), :] = newv[:, 0:128]
            vb[pl.ds(NCB * 256 + 128, 128), :] = newv[:, 128:256]
            for dx in range(1, XD):
                theirs = pl.ds((dx * 2 + 1 - c) * cache, cache)
                for kv, buf in enumerate((kb, vb)):
                    rc(buf.at[theirs], buf.at[theirs], f_ss.at[dx, kv], k_rs.at[dx * 2 + 1 - c, kv], mate).wait_recv()
            blocks_b = list(range(CHB, NKB))
            unit_body(mx, blocks_b, None, NPAIR - 1, False, None)

            def send_unit(p):
                for w in range(1, G):
                    @pl.when(p == (w * UNIT) // 512)
                    def _():
                        for cpy in out_copies(w):
                            cpy.start()

            def pass_b(u, _):
                p = NPAIR - 1 - u
                unit_body(mx, blocks_b, p, p - 1, False, None)
                send_unit(p)
                return 0

            lax.fori_loop(0, NPAIR - 1, pass_b, 0)
            unit_body(mx, blocks_b, 0, None, False, None)
            send_unit(jnp.int32(0))

        def units_for_py(p):
            return min((p * 512 + 511) // UNIT + 1, G)

        def out_copies(w):
            e0 = (w * UNIT) // 128
            return [rc(obuf.at[pl.ds(w * UNIT, UNIT)], orecv.at[w], o_ss.at[w], o_rs.at[w], to_peer(w)),
                    rc(lbuf.at[pl.ds(e0, LSE_ROWS)], lrecv.at[w], l_ss.at[w], l_rs.at[w], to_peer(w))]

        if SIM:
            compute(*([None] * 8))
        else:
            pl.run_scoped(compute, *[pltpu.ACC(t)((128 if a == 3 else 256, 256), F32)
                                     for t in range(2) for a in range(4)])

        for w in range(1, G):
            rc(obuf.at[pl.ds(0, UNIT)], orecv.at[w], o_ss.at[w], o_rs.at[w], mate).wait_recv()
            rc(lbuf.at[pl.ds(0, LSE_ROWS)], lrecv.at[w], l_ss.at[w], l_rs.at[w], mate).wait_recv()
        lane = lax.broadcasted_iota(jnp.int32, (LSE_ROWS, 128), 1)

        def shifted(v, off):
            if off == 0:
                return v
            r = pltpu.roll(v, 128 - off, 1)
            nxt = jnp.concatenate([r[1:], r[-1:]], axis=0)
            return jnp.where(lane[: v.shape[0]] < 128 - off, r, nxt)

        def lse_of(w):
            v = lbuf[pl.ds(0, LSE_ROWS)] if w == 0 else lrecv[w]
            return shifted(v.reshape(LSE_ROWS, 128), (w * UNIT) % 128)

        lses = [lse_of(w) for w in range(G)]
        top = functools.reduce(jnp.maximum, lses)
        wts = [jnp.exp2(v - top) for v in lses]
        den = functools.reduce(jnp.add, wts)
        inv = 1.0 / den
        wts = [v * inv for v in wts]
        total = (top + jnp.log2(den)) * LN2
        pieces = []
        for j in range(-(-UNIT // 128)):
            n = min(128, UNIT - j * 128)
            cols = jnp.concatenate([v[j:j + 1] for v in wts] + [jnp.zeros((128 - G, 128), F32)], axis=0).T
            acc = jnp.zeros((n, 128), F32)
            for w in range(G):
                src = obuf[pl.ds(j * 128, n), :] if w == 0 else orecv[w, pl.ds(j * 128, n), :]
                acc = acc + src.astype(F32) * cols[:n, w:w + 1]
            pieces.append(acc)
        final = jnp.concatenate(pieces, axis=0)
        for i in range(XD):
            fo[i] = final[i * PIECE:(i + 1) * PIECE].astype(BF)
            off = (i * PIECE) % 128
            e = (i * PIECE) // 128
            need = min(3, LSE_ROWS - e)
            v = shifted(total[e:e + need], off)
            v = v if need >= 2 else jnp.concatenate([v, v], axis=0)
            fl[2 * i] = v[0:1]
            fl[2 * i + 1] = v[1:2]
        x_send = []
        for dd in range(1, XD):
            xd = (x + dd) % XD
            x_send.append(rc(fo.at[xd], out.at[x], x_ss.at[dd], x_rs.at[x], x_peer(dd)))
            x_send.append(rc(fl.at[pl.ds(2 * xd, 2)], lse_out.at[pl.ds(2 * x, 2)], y_ss.at[dd], y_rs.at[x], x_peer(dd)))
        for cpy in x_send:
            cpy.start()
        mine = [pltpu.make_async_copy(fo.at[x], out.at[x], lsem.at[0]),
                pltpu.make_async_copy(fl.at[pl.ds(2 * x, 2)], lse_out.at[pl.ds(2 * x, 2)], lsem.at[1])]
        for cpy in mine:
            cpy.start()
        for cpy in q_send + kv_send + n_send + b_send + x_send:
            cpy.wait_send()
        for dx in range(1, XD):
            m = pl.ds((dx * 2 + c) * cache, cache)
            for kv, buf in enumerate((kb, vb)):
                rc(buf.at[m], buf.at[m], f_ss.at[dx, kv], k_rs.at[dx * 2 + c, kv], mate).wait_send()
        for w in range(1, G):
            for cpy in out_copies(w):
                cpy.wait_send()
        for cpy in mine:
            cpy.wait()
        for dd in range(1, XD):
            src = (x + dd) % XD
            rc(fo.at[0], out.at[src], x_ss.at[dd], x_rs.at[src], x_peer(dd)).wait_recv()
            rc(fl.at[pl.ds(0, 2)], lse_out.at[pl.ds(2 * src, 2)], y_ss.at[dd], y_rs.at[src], x_peer(dd)).wait_recv()

    D, R = pltpu.SemaphoreType.DMA, NPAIR * 2
    V = pltpu.VMEM
    scratch = [
        V((NKB * 256, 128), BF), V((NKB * 256, 128), BF), V((NKB * 256, 128), BF),
        V((XD, PIECE, 128), BF), V((NPAIR * 512, 128), BF), V((R, 128, 256), BF),
        V((2, NKB - CHB, 256, 256), F32), V((R, 128, 256), F32),
        V((R, 8, 256), F32), V((R, 8, 256), F32), V((2, 8, 256), F32), V((R, 8, 256), F32),
        V((256, 128), F32), V((8, 2, PAD, 128), BF),
        V((NPAIR * 512, 128), BF), V((R * 2 + LSE_ROWS, 1, 128), F32),
        V((G, UNIT, 128), BF), V((G, LSE_ROWS, 1, 128), F32),
        V((XD, PIECE, 128), BF), V((2 * XD, 1, 128), F32),
        D((5,)), D((XD,)), D((XD,)), D((G,)), D((G,)), D((XD, 2)), D((2 * XD, 2)), D((XD, 2)), D((7,)), D((8,)),
        D((G,)), D((G,)), D((G,)), D((G,)), D((XD,)), D((XD,)), D((XD,)), D((XD,)),
    ]
    any_ = pl.BlockSpec(memory_space=pl.ANY)
    return pl.pallas_call(
        kernel,
        out_shape=(jax.ShapeDtypeStruct((XD, PIECE, 128), BF), jax.ShapeDtypeStruct((2 * XD, 1, 128), F32)),
        in_specs=[pl.BlockSpec(memory_space=pltpu.SMEM)] + [any_] * 5,
        out_specs=(any_, any_),
        scratch_shapes=scratch,
        name="prefix_attention",
        compiler_params=pltpu.CompilerParams(collective_id=0, has_side_effects=True, vmem_limit_bytes=63 << 20),
    ), (offs, G, PIECE, UNIT, ROWS, NPAIR)


def solution(mesh):
    spec = P(("dp", "cp"))

    def local(queries, key_new, value_new, key_cache, value_cache, prefix_len):
        tok, cache = queries.shape[0], key_cache.shape[0]
        call, (offs, G, PIECE, UNIT, ROWS, NPAIR) = make_kernel(tok, cache)
        cp = lax.axis_index("cp")
        c, y, z = cp % 2, (cp // (2 * XD)) % YD, cp // (2 * XD * YD)
        q = queries.transpose(1, 0, 2).reshape(KV, PIECE, HD)
        k = key_cache.transpose(1, 0, 2)
        v = value_cache.reshape(cache // 128, 128, KV, HD).transpose(2, 0, 3, 1).reshape(KV, cache, 128)
        new = jnp.stack([key_new.transpose(1, 0, 2), value_new.transpose(1, 0, 2)], axis=1)
        new = jnp.pad(new, ((0, 0), (0, 0), (0, PAD - tok), (0, 0)))
        dy = jnp.array([o[0] for o in offs], jnp.int32)
        dz = jnp.array([o[1] for o in offs], jnp.int32)
        chip_row = (((z + dz) % ZD) * YD + (y + dy) % YD) * XD
        dev = (chip_row[:, None] + jnp.arange(XD)[None, :]) * 2 + c
        token = dev[:, :, None, None] * tok + jnp.arange(tok)[None, None, None, :]
        token = jnp.broadcast_to(token, (G, XD, RATIO, tok)).reshape(ROWS)
        token = jnp.pad(token, (0, NPAIR * 512 - ROWS)).astype(F32)
        tq = jnp.broadcast_to(token.reshape(NPAIR * 2, 1, 256), (NPAIR * 2, 8, 256))
        out, lse = call(prefix_len, q, k, v, new, tq)
        attn_out = out.reshape(HEADS, tok, HD).transpose(1, 0, 2)
        row_lse = lse.reshape(KV, 256)[:, :PIECE].reshape(HEADS, tok).T
        return attn_out, row_lse

    return jax.shard_map(local, mesh=mesh, in_specs=(spec,) * 5 + (P("dp"),), out_specs=(spec, spec), check_vma=False)
```

```python
import functools
import math

import jax
import jax.numpy as jnp
from jax import lax
from jax.experimental import pallas as pl
from jax.experimental.pallas import tpu as pltpu
from jax.sharding import PartitionSpec as P

ZD, YD, XD = 4, 4, 4

HEADS, KV, HD = 28, 4, 128
RATIO = HEADS // KV
FILL = -1e30
SCALE2 = HD ** -0.5 * math.log2(math.e)
LN2 = math.log(2.0)
PAD = 32
BF, F32 = jnp.bfloat16, jnp.float32


def ring_offsets():
    def hops(d, n):
        return min(d, n - d)

    offs = [(dy, dz) for dz in range(ZD) for dy in range(YD)]
    return sorted(offs, key=lambda o: (hops(o[0], YD) + hops(o[1], ZD), o[1], o[0]))


def make_kernel(tok, cache):
    offs = ring_offsets()
    G = len(offs)
    PIECE = RATIO * tok
    UNIT = XD * PIECE
    ROWS = G * UNIT
    NPAIR = -(-ROWS // 512)
    CHB = 2 * cache // 256
    NCB = XD * CHB
    NKB = NCB + 1
    HALF = (UNIT // 2 + 31) // 32 * 32 if UNIT > 512 else UNIT // 2
    SIZE = (HALF, UNIT - HALF)
    assert HALF % 16 == 0 and UNIT % 16 == 0
    slot_of = {o: w for w, o in enumerate(offs)}
    relayed = {w for w, (dy, dz) in enumerate(offs) if (YD == 4 and dy == 2) != (ZD == 4 and dz == 2)}
    onward = []
    for w, (dy, dz) in enumerate(offs):
        if w and w not in relayed and (dy, dz) != (2, 2):
            if YD == 4 and dy in (1, 3):
                onward.append((2 * w + (dy == 3), (-1 if dy == 1 else 1), 0, slot_of[2, dz]))
            if ZD == 4 and dz in (1, 3):
                onward.append((2 * w + (dz == 3), 0, (-1 if dz == 1 else 1), slot_of[dy, 2]))
    direct = [w for w in range(1, G) if w not in relayed]
    LSE_ROWS = UNIT // 128 + 1
    assert cache % 256 == 0 and 8 * PAD == 256 and tok <= PAD

    def kernel(plen, q_in, k_in, v_in, kn_in, vn_in, out, lse_out,
               qv, kraw, vraw, knraw, vnraw, kh, vh, nh, rk, rv,
               kb, vb, bias, qx, qall, qt, sb, oacc, mb, lb, mcur, oraw, lraw, mraw, tq, keyid, nrecv,
               obuf, lbuf, orecv, lrecv, fo, fl, flr,
               lsem, q_ss, q_rs, b_ss, b_rs, w_ss, k_ss, k_rs, f_ss, r_ss, r_rs, h_ss, n_ss, n_rs,
               o_ss, o_rs, l_ss, l_rs, x_ss, x_rs, y_ss, y_rs):
        cp = lax.axis_index("cp")
        c = cp % 2
        x = (cp // 2) % XD
        y = (cp // (2 * XD)) % YD
        z = cp // (2 * XD * YD)
        row0 = (z * YD + y) * XD

        def at(xx, yy, zz, cc):
            return ((zz * YD + yy) * XD + xx) * 2 + cc

        def x_peer(dd):
            return at((x + dd) % XD, y, z, c)

        mate = at(x, y, z, 1 - c)

        def to_peer(w):
            dy, dz = offs[w]
            return at(x, (y + dy) % YD, (z + dz) % ZD, c)

        def from_peer(w):
            dy, dz = offs[w]
            return at(x, (y + YD - dy) % YD, (z + ZD - dz) % ZD, c)

        def rc(src, dst, ss, rs, dev):
            return pltpu.make_async_remote_copy(
                src_ref=src, dst_ref=dst, send_sem=ss, recv_sem=rs,
                device_id={"cp": dev}, device_id_type=pl.DeviceIdType.MESH)

        row_devs = [(dd, dc) for dd in range(XD) for dc in range(2) if (dd, dc) != (0, 0)]

        def row_peer(dd, dc):
            return at((x + dd) % XD, y, z, (c + dc) % 2)

        barrier = pltpu.get_barrier_semaphore()
        peers = [to_peer(w) for w in range(1, G)] + [row_peer(dd, dc) for dd, dc in row_devs]
        for p in peers:
            pl.semaphore_signal(barrier, inc=1, device_id={"cp": p}, device_id_type=pl.DeviceIdType.MESH)
        me_j = x * 2 + c
        own = pl.ds(c * cache, cache)
        local = [pltpu.make_async_copy(src, dst, lsem.at[i]) for i, (src, dst) in enumerate(
            [(q_in, qv), (k_in, kraw), (v_in, vraw), (kn_in, knraw), (vn_in, vnraw)])]
        for cpy in local:
            cpy.start()
        local[0].wait()
        pl.semaphore_wait(barrier, len(peers))

        q_send = [rc(qv.at[(x + dd) % XD], qx.at[x], q_ss.at[dd], q_rs.at[x], x_peer(dd)) for dd in range(1, XD)]
        for cpy in q_send:
            cpy.start()

        def iota(shape, d):
            return lax.broadcasted_iota(jnp.int32, shape, d)

        i0, i1 = iota((256, 256), 0), iota((256, 256), 1)
        pick = jnp.where(i1 == (i0 & 63) * KV + lax.shift_right_logical(i0, 6), 1.0, 0.0).astype(BF)
        for cpy in local[1:]:
            cpy.wait()
        groups = cache // 128
        unroll = max(u for u in (1, 2, 4) if groups % u == 0)

        def split(g0, _):
            for du in range(unroll):
                g = g0 * unroll + du
                for raw, dst, flip in ((kraw, kh, False), (vraw, vh, True)):
                    rows = raw[pl.ds(pl.multiple_of(g * 128 * KV, 256), 128 * KV), :]
                    both = jnp.concatenate([rows[:256], rows[256:]], axis=1)
                    r = jnp.dot(pick, both, preferred_element_type=F32).astype(BF)
                    for h in range(KV):
                        one = jnp.concatenate([r[h * 64:(h + 1) * 64, :128], r[h * 64:(h + 1) * 64, 128:]], axis=0)
                        dst[h, pl.ds(pl.multiple_of(g * 128, 128), 128), :] = one.T if flip else one
            return 0

        lax.fori_loop(0, groups // unroll, split, 0)
        kb[own, :] = kh[x]
        vb[own, :] = vh[x]
        n0, n1 = iota((KV * PAD, tok * KV), 0), iota((KV * PAD, tok * KV), 1)
        npick = jnp.where((n0 % PAD < tok) & (n1 == (n0 % PAD) * KV + n0 // PAD), 1.0, 0.0).astype(BF)
        for i, raw in enumerate((knraw, vnraw)):
            r = jnp.dot(npick, raw[...], preferred_element_type=F32).astype(BF)
            for h in range(KV):
                nh[h, i] = r[h * PAD:(h + 1) * PAD]
        nrecv[me_j] = nh[x]

        def kv_copies(dd):
            slot = ((XD - dd) % XD) * 2 + c
            there = pl.ds(slot * cache, cache)
            dev = x_peer(dd) if dd else mate
            return [rc(src.at[(x + dd) % XD], dst.at[there], k_ss.at[dd, i], k_rs.at[slot, i], dev)
                    for i, (src, dst) in enumerate(((kh, kb), (vh, vb)))]

        kv_send = kv_copies(0)
        kv_send += [rc(kh.at[(x + 2) % XD], rk, r_ss.at[0], r_rs.at[0], x_peer(1)),
                    rc(vh.at[(x + 2) % XD], rv, r_ss.at[1], r_rs.at[1], x_peer(3))]
        kv_send += kv_copies(1) + kv_copies(3)
        n_send = [rc(nh.at[(x + dd) % XD], nrecv.at[me_j], n_ss.at[i], n_rs.at[me_j], row_peer(dd, dc))
                  for i, (dd, dc) in enumerate(row_devs)]
        for cpy in kv_send + n_send:
            cpy.start()
        there = pl.ds((2 * 2 + c) * cache, cache)
        kv_relay = [rc(rk, kb.at[there], h_ss.at[0], k_rs.at[2 * 2 + c, 0], x_peer(1)),
                    rc(rv, vb.at[there], h_ss.at[1], k_rs.at[2 * 2 + c, 1], x_peer(3))]

        for dd in range(1, XD):
            src = (x + dd) % XD
            rc(qv.at[x], qx.at[src], q_ss.at[dd], q_rs.at[src], x_peer(dd)).wait_recv()

        def joined(pieces):
            return jnp.concatenate([v.astype(F32) for v in pieces], axis=0).astype(BF)

        qx[x] = qv[x]
        qall[pl.ds(0, UNIT), :] = joined([qx[i] for i in range(XD)])
        def half(w, h):
            start = w * UNIT + h * HALF
            return pl.ds(start if isinstance(w, int) else pl.multiple_of(start, 16), SIZE[h])

        b_send = [rc(qall.at[half(0, h)], qall.at[half(w, h)], b_ss.at[2 * w + h], b_rs.at[2 * w + h], from_peer(w))
                  for w in direct for h in range(2)]
        for cpy in b_send:
            cpy.start()
        w_send = []
        for i, (hw, sy, sz, there_w) in enumerate(onward):
            w, h = hw // 2, hw % 2
            dev = at(x, (y + YD + sy) % YD, (z + ZD + sz) % ZD, c)
            w_send.append(rc(qall.at[half(w, h)], qall.at[half(there_w, h)], w_ss.at[i], b_rs.at[2 * there_w + h], dev))

        prefix = plen[0]
        riota = iota((256, 128), 0)
        lane0 = iota((256, 128), 1) == 0
        nblk = cache // 256

        def bias_block(b, _):
            slot = b // nblk
            base = ((row0 + (x + slot // 2) % XD) * 2 + slot % 2) * cache + (b % nblk) * 256
            hide = jnp.where(lane0 & (riota + base >= prefix), FILL, 0.0)
            bias[pl.ds(pl.multiple_of(b * 256, 256), 256), :] = hide.astype(BF)
            return 0

        lax.fori_loop(0, NCB, bias_block, 0)
        bias[pl.ds(NCB * 256, 256), :] = jnp.zeros((256, 128), BF)
        dev_j = lax.shift_right_logical(riota, 5)
        r_j = lax.bitwise_and(riota, PAD - 1)
        keyid[...] = jnp.where(r_j < tok, (row0 * 2 + dev_j) * tok + r_j, 1 << 23).astype(F32)

        r = (iota((NPAIR * 2, 256), 0) * 256 + iota((NPAIR * 2, 256), 1)).astype(F32)

        def parts(v, n):
            d = jnp.floor((v + 0.5) * (1.0 / n))
            return d, v - d * n

        unit_no, rest = parts(r, UNIT)
        chip_no, rest = parts(rest, PIECE)
        _, tok_no = parts(rest, tok)
        chip_row = jnp.zeros_like(r)
        for w, (dy, dz) in enumerate(offs):
            first_chip = ((z + dz) % ZD * YD + (y + dy) % YD) * XD
            chip_row = jnp.where(unit_no == w, first_chip.astype(F32), chip_row)
        tq[...] = ((chip_row + chip_no) * 2.0 + c.astype(F32)) * tok + tok_no

        def wait_half(hw, _):
            for h in range(2):
                @pl.when(hw % 2 == h)
                def _():
                    rc(qall.at[half(0, h)], qall.at[half(hw // 2, h)], b_ss.at[hw], b_rs.at[hw], mate).wait_recv()

            for i, (k, *_) in enumerate(onward):
                @pl.when(hw == k)
                def _():
                    w_send[i].start()

            return 0

        def halves_for(p):
            last = p * 512 + 511
            n = last // UNIT * 2 + 1 + (last % UNIT >= HALF)
            return min(n, 2 * G) if isinstance(p, int) else jnp.minimum(n, 2 * G)

        def prep(p):
            for t in range(2):
                rows = qall[pl.ds(pl.multiple_of((p * 2 + t) * 256, 256), 256), :]
                qt[p * 2 + t] = rows.T

        ones_row = jnp.where(iota((128, 256), 0) == 0, 1.0, 0.0).astype(BF)

        def rep(v, n):
            return jnp.concatenate([v] * n, axis=0)

        def finish(p):
            for t in range(2):
                tile = p * 2 + t
                m = mraw[t]
                alpha = jnp.exp2((mb[tile] - m) * SCALE2)
                l = jnp.sum(lraw[t] + alpha * lb[tile], axis=0, keepdims=True)
                inv = 1.0 / l
                o = (oacc[tile] * rep(alpha, 16) + oraw[t]) * inv
                obuf[pl.ds(pl.multiple_of(tile * 256, 256), 256), :] = o.T.astype(BF)
                ls = m[0:1] * SCALE2 + jnp.log2(l)
                lbuf[tile * 2] = ls[:, 0:128]
                lbuf[tile * 2 + 1] = ls[:, 128:256]

        blocks_a = list(range(CHB))
        blocks_b = list(range(CHB, NKB))

        def unit_body(pv=None, pv_first=True, qk=None, qk_first=True, prep_pair=None, done_pair=None):
            pv_blocks = [] if pv is None else blocks_a if pv_first else blocks_b
            qk_blocks = [] if qk is None else blocks_a if qk_first else blocks_b
            if done_pair is not None:
                finish(done_pair)
            mp = [mcur[t] for t in range(2)]
            lacc = [jnp.zeros((8, 256), F32) for _ in range(2)]
            o = [None, None]
            mxs = [jnp.full((8, 256), -jnp.inf, F32) for _ in range(2)]

            def scores(b, t):
                k = jnp.concatenate([kb[pl.ds(b * 256, 256), :], bias[pl.ds(b * 256, 256), :]], axis=1)
                q = jnp.concatenate([qt[qk * 2 + t], ones_row], axis=0)
                return jnp.dot(k, q, preferred_element_type=F32)

            def keep(i, b, t, s):
                if b == NCB:
                    lim = tq[pl.ds(qk * 2 + t, 1), :]
                    kid = jnp.concatenate([keyid[...], keyid[...]], axis=1)
                    s = jnp.where(kid <= lim, s, FILL)
                sb[t, i] = s
                mxs[t] = jnp.maximum(mxs[t], s.reshape(32, 8, 256).max(0))

            def weigh(i, b, t):
                p = jnp.exp2((sb[t, i] - rep(mp[t], 32)) * SCALE2)
                lacc[t] = lacc[t] + p.reshape(32, 8, 256).sum(0)
                vt = jnp.concatenate([vb[pl.ds(b * 256, 128), :], vb[pl.ds(b * 256 + 128, 128), :]], axis=1)
                d = jnp.dot(vt, p.astype(BF), preferred_element_type=F32)
                o[t] = d if o[t] is None else o[t] + d

            for i in range(max(len(pv_blocks), len(qk_blocks))):
                for t in range(2):
                    if i < len(qk_blocks) and t == 0:
                        s = scores(qk_blocks[i], t)
                    if i < len(pv_blocks):
                        weigh(i, pv_blocks[i], t)
                    if i < len(qk_blocks):
                        keep(i, qk_blocks[i], t, s if t == 0 else scores(qk_blocks[i], t))
            if pv is not None:
                for t in range(2):
                    tile = pv * 2 + t
                    if pv_first:
                        oacc[tile] = o[t]
                        lb[tile] = lacc[t]
                    else:
                        oraw[t] = o[t]
                        lraw[t] = lacc[t]
                        mraw[t] = mp[t]
            if prep_pair is not None:
                prep(prep_pair)
            if qk is not None:
                for t in range(2):
                    m = jnp.broadcast_to(jnp.max(mxs[t], axis=0, keepdims=True), (8, 256))
                    if qk_first:
                        mb[qk * 2 + t] = m
                    else:
                        m = jnp.maximum(m, mb[qk * 2 + t])
                    mcur[t] = m

        def compute():
            other = pl.ds((1 - c) * cache, cache)
            for i, (src, dst) in enumerate(((kh, kb), (vh, vb))):
                rc(src.at[x], dst.at[other], k_ss.at[0, i], k_rs.at[1 - c, i], mate).wait_recv()
            prep(0)
            unit_body(qk=0)
            for hw in range(2, halves_for(min(1, NPAIR - 1))):
                wait_half(jnp.int32(hw), 0)
            prep(1)

            def forwarded(dx, cc):
                there = pl.ds((dx * 2 + cc) * cache, cache)
                return [rc(buf.at[there], buf.at[there], f_ss.at[dx, i], k_rs.at[dx * 2 + cc, i], mate)
                        for i, buf in enumerate((kb, vb))]

            def forward(dxs):
                for dx in dxs:
                    for cpy in forwarded(dx, c):
                        cpy.wait_recv()
                        cpy.start()

            def pass_a(u, _):
                lax.fori_loop(halves_for(u + 1), halves_for(u + 2), wait_half, 0)

                @pl.when(u == min(3, NPAIR - 2))
                def _():
                    for i, buf in enumerate((rk, rv)):
                        rc(buf, buf, r_ss.at[i], r_rs.at[i], mate).wait_recv()
                        kv_relay[i].start()

                @pl.when(u == min(14, NPAIR - 2))
                def _():
                    forward((1, 3))

                @pl.when(u == NPAIR - 2)
                def _():
                    forward((2,))

                unit_body(pv=u, qk=u + 1, prep_pair=jnp.minimum(u + 2, NPAIR - 1))
                return 0

            unit_body(pv=0, qk=1)
            lax.fori_loop(halves_for(1), halves_for(2), wait_half, 0)
            prep(2)
            lax.fori_loop(1, NPAIR - 1, pass_a, 0)

            for i in range(1, 8):
                j = (me_j + i) % 8
                rc(nh.at[x], nrecv.at[j], n_ss.at[0], n_rs.at[j], mate).wait_recv()
            newv = jnp.concatenate([nrecv[j, 1] for j in range(8)], axis=0).T
            kb[pl.ds(NCB * 256, 256), :] = jnp.concatenate([nrecv[j, 0] for j in range(8)], axis=0)
            vb[pl.ds(NCB * 256, 128), :] = newv[:, 0:128]
            vb[pl.ds(NCB * 256 + 128, 128), :] = newv[:, 128:256]
            for dx in range(1, XD):
                for cpy in forwarded(dx, 1 - c):
                    cpy.wait_recv()
            unit_body(pv=NPAIR - 1, qk=NPAIR - 1, qk_first=False)

            def send_unit(p):
                for w in range(1, G):
                    @pl.when(p == (w * UNIT) // 512)
                    def _():
                        for cpy in out_copies(w):
                            cpy.start()

            def pass_b(u, _):
                p = NPAIR - 1 - u
                unit_body(pv=p, pv_first=False, qk=p - 1, qk_first=False, done_pair=jnp.minimum(p + 1, NPAIR - 1))
                send_unit(p + 1)
                return 0

            lax.fori_loop(0, NPAIR - 1, pass_b, 0)
            finish(1)
            send_unit(jnp.int32(1))
            unit_body(pv=0, pv_first=False)
            finish(0)
            send_unit(jnp.int32(0))

        def out_copies(w):
            e0 = (w * UNIT) // 128
            return [rc(obuf.at[pl.ds(w * UNIT, UNIT)], orecv.at[w], o_ss.at[w], o_rs.at[w], to_peer(w)),
                    rc(lbuf.at[pl.ds(e0, LSE_ROWS)], lrecv.at[w], l_ss.at[w], l_rs.at[w], to_peer(w))]

        compute()

        for w in range(1, G):
            rc(obuf.at[pl.ds(0, UNIT)], orecv.at[w], o_ss.at[w], o_rs.at[w], mate).wait_recv()
            rc(lbuf.at[pl.ds(0, LSE_ROWS)], lrecv.at[w], l_ss.at[w], l_rs.at[w], mate).wait_recv()
        lane = iota((LSE_ROWS, 128), 1)

        def shifted(v, off):
            if off == 0:
                return v
            r = pltpu.roll(v, 128 - off, 1)
            nxt = jnp.concatenate([r[1:], r[-1:]], axis=0)
            return jnp.where(lane[: v.shape[0]] < 128 - off, r, nxt)

        def lse_of(w):
            v = lbuf[pl.ds(0, LSE_ROWS)] if w == 0 else lrecv[w]
            return shifted(v.reshape(LSE_ROWS, 128), (w * UNIT) % 128)

        lses = [lse_of(w) for w in range(G)]
        top = functools.reduce(jnp.maximum, lses)
        wts = [jnp.exp2(v - top) for v in lses]
        den = functools.reduce(jnp.add, wts)
        inv = 1.0 / den
        wts = [v * inv for v in wts]
        total = (top + jnp.log2(den)) * LN2
        pieces = []
        for j in range(-(-UNIT // 128)):
            n = min(128, UNIT - j * 128)
            cols = jnp.concatenate([v[j:j + 1] for v in wts] + [jnp.zeros((128 - G, 128), F32)], axis=0).T
            acc = jnp.zeros((n, 128), F32)
            for w in range(G):
                src = obuf[pl.ds(j * 128, n), :] if w == 0 else orecv[w, pl.ds(j * 128, n), :]
                acc = acc + src.astype(F32) * cols[:n, w:w + 1]
            pieces.append(acc)
        final = jnp.concatenate(pieces, axis=0)
        for i in range(XD):
            fo[i] = final[i * PIECE:(i + 1) * PIECE].astype(BF)
            off = (i * PIECE) % 128
            e = (i * PIECE) // 128
            need = min(3, LSE_ROWS - e)
            v = shifted(total[e:e + need], off)
            v = v if need >= 2 else jnp.concatenate([v, v], axis=0)
            fl[2 * i] = v[0:1]
            fl[2 * i + 1] = v[1:2]
        x_send = []
        for dd in range(1, XD):
            xd = (x + dd) % XD
            x_send.append(rc(fo.at[xd], out.at[x], x_ss.at[dd], x_rs.at[x], x_peer(dd)))
            x_send.append(rc(fl.at[pl.ds(2 * xd, 2)], flr.at[pl.ds(2 * x, 2)], y_ss.at[dd], y_rs.at[x], x_peer(dd)))
        for cpy in x_send:
            cpy.start()
        mine = pltpu.make_async_copy(fo.at[x], out.at[x], lsem.at[0])
        mine.start()
        flr[pl.ds(2 * x, 2)] = fl[pl.ds(2 * x, 2)]
        for cpy in q_send + kv_send + kv_relay + n_send + b_send + w_send + x_send:
            cpy.wait_send()
        for dx in range(1, XD):
            m = pl.ds((dx * 2 + c) * cache, cache)
            for i, buf in enumerate((kb, vb)):
                rc(buf.at[m], buf.at[m], f_ss.at[dx, i], k_rs.at[dx * 2 + c, i], mate).wait_send()
        for w in range(1, G):
            for cpy in out_copies(w):
                cpy.wait_send()
        mine.wait()
        for dd in range(1, XD):
            src = (x + dd) % XD
            rc(fl.at[pl.ds(0, 2)], flr.at[pl.ds(2 * src, 2)], y_ss.at[dd], y_rs.at[src], x_peer(dd)).wait_recv()
        head_rows = []
        for i in range(KV):
            pair = flr[pl.ds(2 * i, 2)].reshape(2, 128)
            for g in range(RATIO):
                s = g * tok
                lo = pair[s // 128:s // 128 + 1]
                head_rows.append(lo if s % 128 == 0 else jnp.where(
                    lane[:1] < 128 - s % 128, pltpu.roll(lo, 128 - s % 128, 1), pltpu.roll(pair[1:2], 128 - s % 128, 1)))
        table = jnp.concatenate(head_rows + [jnp.zeros((32 - HEADS, 128), F32)], axis=0).T
        lse_out[...] = table[:tok, :HEADS]
        for dd in range(1, XD):
            src = (x + dd) % XD
            rc(fo.at[0], out.at[src], x_ss.at[dd], x_rs.at[src], x_peer(dd)).wait_recv()

    D, R = pltpu.SemaphoreType.DMA, NPAIR * 2
    V = pltpu.VMEM
    scratch = [
        V((XD, PIECE, 128), BF), V((cache * KV, 128), BF), V((cache * KV, 128), BF),
        V((tok * KV, 128), BF), V((tok * KV, 128), BF),
        V((KV, cache, 128), BF), V((KV, cache, 128), BF), V((KV, 2, PAD, 128), BF),
        V((cache, 128), BF), V((cache, 128), BF),
        V((NKB * 256, 128), BF), V((NKB * 256, 128), BF), V((NKB * 256, 128), BF),
        V((XD, PIECE, 128), BF),
        V((NPAIR * 512, 128), BF), V((R, 128, 256), BF),
        V((2, NKB - CHB, 256, 256), F32), V((R, 128, 256), F32),
        V((R, 8, 256), F32), V((R, 8, 256), F32), V((2, 8, 256), F32),
        V((2, 128, 256), F32), V((2, 8, 256), F32), V((2, 8, 256), F32), V((R, 256), F32),
        V((256, 128), F32), V((8, 2, PAD, 128), BF),
        V((NPAIR * 512, 128), BF), V((R * 2 + LSE_ROWS, 1, 128), F32),
        V((G, UNIT, 128), BF), V((G, LSE_ROWS, 1, 128), F32),
        V((XD, PIECE, 128), BF), V((2 * XD, 1, 128), F32), V((2 * XD, 1, 128), F32),
        D((5,)), D((XD,)), D((XD,)), D((2 * G,)), D((2 * G,)), D((max(1, len(onward)),)),
        D((XD, 2)), D((2 * XD, 2)), D((XD, 2)), D((2,)), D((2,)), D((2,)), D((7,)), D((8,)),
        D((G,)), D((G,)), D((G,)), D((G,)), D((XD,)), D((XD,)), D((XD,)), D((XD,)),
    ]
    any_ = pl.BlockSpec(memory_space=pl.ANY)
    return pl.pallas_call(
        kernel,
        out_shape=(jax.ShapeDtypeStruct((XD, PIECE, 128), BF), jax.ShapeDtypeStruct((tok, HEADS), F32)),
        in_specs=[pl.BlockSpec(memory_space=pltpu.SMEM)] + [any_] * 5,
        out_specs=(any_, pl.BlockSpec(memory_space=pltpu.VMEM)),
        scratch_shapes=scratch,
        name="prefix_attention",
        compiler_params=pltpu.CompilerParams(collective_id=0, has_side_effects=True, vmem_limit_bytes=63 << 20),
    )


def solution(mesh):
    spec = P(("dp", "cp"))

    def local(queries, key_new, value_new, key_cache, value_cache, prefix_len):
        tok, cache = queries.shape[0], key_cache.shape[0]
        call = make_kernel(tok, cache)
        q = queries.transpose(1, 0, 2).reshape(KV, RATIO * tok, HD)

        def rows(a):
            return a.reshape(a.shape[0] * KV, HD)

        out, row_lse = call(prefix_len, q, rows(key_cache), rows(value_cache), rows(key_new), rows(value_new))
        return out.reshape(HEADS, tok, HD).transpose(1, 0, 2), row_lse

    return jax.shard_map(local, mesh=mesh, in_specs=(spec,) * 5 + (P("dp"),), out_specs=(spec, spec), check_vma=False)
```

```python
import functools
import math

import jax
import jax.numpy as jnp
from jax import lax
from jax.experimental import pallas as pl
from jax.experimental.pallas import tpu as pltpu
from jax.sharding import PartitionSpec as P

ZD, YD, XD = 4, 4, 4

HEADS, KV, HD = 28, 4, 128
RATIO = HEADS // KV
FILL = -1e30
SCALE2 = HD ** -0.5 * math.log2(math.e)
LN2 = math.log(2.0)
PAD = 32
BF, F32 = jnp.bfloat16, jnp.float32


def ring_offsets():
    def hops(d, n):
        return min(d, n - d)

    offs = [(dy, dz) for dz in range(ZD) for dy in range(YD)]
    return sorted(offs, key=lambda o: (hops(o[0], YD) + hops(o[1], ZD), 0 in o, o[1], o[0]))


def on_value(v, actions):
    keys = sorted(actions)
    if len(keys) == 1:
        pl.when(v == keys[0])(actions[keys[0]])
    elif keys:
        mid = keys[len(keys) // 2]
        pl.when(v < mid)(lambda: on_value(v, {k: a for k, a in actions.items() if k < mid}))
        pl.when(v >= mid)(lambda: on_value(v, {k: a for k, a in actions.items() if k >= mid}))


def make_kernel(tok, cache):
    offs = ring_offsets()
    G = len(offs)
    PIECE = RATIO * tok
    UNIT = XD * PIECE
    ROWS = G * UNIT
    NPAIR = -(-ROWS // 512)
    CHB = 2 * cache // 256
    NCB = XD * CHB
    NKB = NCB + 1
    HALF = (UNIT // 2 + 31) // 32 * 32 if UNIT > 512 else UNIT // 2
    SIZE = (HALF, UNIT - HALF)
    assert HALF % 16 == 0 and UNIT % 16 == 0
    slot_of = {o: w for w, o in enumerate(offs)}
    straight = [w for w, o in enumerate(offs) if w and 0 in o and 2 not in o]
    late = [w for w, o in enumerate(offs) if o == (2, 2)]
    assert straight == list(range(1, len(straight) + 1))

    def toward(d, n):
        return 1 if d <= n // 2 else -1

    onward = []
    for w, (ty, tz) in enumerate(offs):
        if w == 0 or w in straight or w in late:
            continue
        if YD == 4 and ty == 2:
            via = [(1, 0), (-1, 0)]
        elif ZD == 4 and tz == 2:
            via = [(0, 1), (0, -1)]
        else:
            via = [(toward(ty, YD), 0), (0, toward(tz, ZD))]
        for h, (ny, nz) in enumerate(via):
            onward.append((2 * slot_of[(ty - ny) % YD, (tz - nz) % ZD] + h, -ny, -nz, w))
    onward.sort()
    NEAR_END = 2 * (len(straight) + 1)
    LSE_ROWS = UNIT // 128 + 1
    assert cache % 256 == 0 and 8 * PAD == 256 and tok <= PAD

    def kernel(plen, q_in, k_in, v_in, kn_in, vn_in, out, lse_out,
               qv, kraw, vraw, knraw, vnraw, kh, vh, nh, rk, rv,
               kb, vb, bias, qx, qall, qt, sb, oacc, mb, lb, mcur, oraw, lraw, mraw, tq, keyid, nrecv,
               obuf, lbuf, orecv, lrecv, fo, fl, flr, ltab,
               lsem, q_ss, q_rs, b_ss, b_rs, w_ss, k_ss, k_rs, f_ss, r_ss, r_rs, h_ss, n_ss, n_rs,
               o_ss, o_rs, l_ss, l_rs, x_ss, x_rs, y_ss, y_rs):
        cp = lax.axis_index("cp")
        c = cp % 2
        x = (cp // 2) % XD
        y = (cp // (2 * XD)) % YD
        z = cp // (2 * XD * YD)
        row0 = (z * YD + y) * XD

        def at(xx, yy, zz, cc):
            return ((zz * YD + yy) * XD + xx) * 2 + cc

        def x_peer(dd):
            return at((x + dd) % XD, y, z, c)

        mate = at(x, y, z, 1 - c)

        def to_peer(w):
            dy, dz = offs[w]
            return at(x, (y + dy) % YD, (z + dz) % ZD, c)

        def from_peer(w):
            dy, dz = offs[w]
            return at(x, (y + YD - dy) % YD, (z + ZD - dz) % ZD, c)

        def start_all(cpys):
            for cpy in cpys:
                cpy.start()

        def rc(src, dst, ss, rs, dev):
            return pltpu.make_async_remote_copy(
                src_ref=src, dst_ref=dst, send_sem=ss, recv_sem=rs,
                device_id={"cp": dev}, device_id_type=pl.DeviceIdType.MESH)

        row_devs = [(dd, dc) for dd in range(XD) for dc in range(2) if (dd, dc) != (0, 0)]

        def row_peer(dd, dc):
            return at((x + dd) % XD, y, z, (c + dc) % 2)

        barrier = pltpu.get_barrier_semaphore()
        peers = [to_peer(w) for w in range(1, G)] + [row_peer(dd, dc) for dd, dc in row_devs]
        for p in peers:
            pl.semaphore_signal(barrier, inc=1, device_id={"cp": p}, device_id_type=pl.DeviceIdType.MESH)
        me_j = x * 2 + c
        own = pl.ds(c * cache, cache)
        local = [pltpu.make_async_copy(src, dst, lsem.at[i]) for i, (src, dst) in enumerate(
            [(q_in, qv), (k_in, kraw), (v_in, vraw), (kn_in, knraw), (vn_in, vnraw)])]
        for cpy in local:
            cpy.start()
        local[0].wait()
        pl.semaphore_wait(barrier, len(peers))

        q_send = [rc(qv.at[(x + dd) % XD], qx.at[x], q_ss.at[dd], q_rs.at[x], x_peer(dd)) for dd in (2, 1, 3)]
        start_all(q_send)

        def iota(shape, d):
            return lax.broadcasted_iota(jnp.int32, shape, d)

        i0, i1 = iota((256, 256), 0), iota((256, 256), 1)
        pick = jnp.where(i1 == (i0 & 63) * KV + lax.shift_right_logical(i0, 6), 1.0, 0.0).astype(BF)
        for cpy in local[1:]:
            cpy.wait()
        groups = cache // 128
        unroll = max(u for u in (1, 2, 4) if groups % u == 0)

        def split(g0, _):
            for du in range(unroll):
                g = g0 * unroll + du
                for raw, dst, flip in ((kraw, kh, False), (vraw, vh, True)):
                    rows = raw[pl.ds(pl.multiple_of(g * 128 * KV, 256), 128 * KV), :]
                    both = jnp.concatenate([rows[:256], rows[256:]], axis=1)
                    r = jnp.dot(pick, both, preferred_element_type=F32).astype(BF)
                    for h in range(KV):
                        one = jnp.concatenate([r[h * 64:(h + 1) * 64, :128], r[h * 64:(h + 1) * 64, 128:]], axis=0)
                        dst[h, pl.ds(pl.multiple_of(g * 128, 128), 128), :] = one.T if flip else one
            return 0

        lax.fori_loop(0, groups // unroll, split, 0)
        kb[own, :] = kh[x]
        vb[own, :] = vh[x]
        n0, n1 = iota((KV * PAD, tok * KV), 0), iota((KV * PAD, tok * KV), 1)
        npick = jnp.where((n0 % PAD < tok) & (n1 == (n0 % PAD) * KV + n0 // PAD), 1.0, 0.0).astype(BF)
        for i, raw in enumerate((knraw, vnraw)):
            r = jnp.dot(npick, raw[...], preferred_element_type=F32).astype(BF)
            for h in range(KV):
                nh[h, i] = r[h * PAD:(h + 1) * PAD]
        nrecv[me_j] = nh[x]

        def kv_copies(dd):
            slot = ((XD - dd) % XD) * 2 + c
            there = pl.ds(slot * cache, cache)
            dev = x_peer(dd) if dd else mate
            return [rc(src.at[(x + dd) % XD], dst.at[there], k_ss.at[dd, i], k_rs.at[slot, i], dev)
                    for i, (src, dst) in enumerate(((kh, kb), (vh, vb)))]

        kv_send = kv_copies(0)
        kv_send += [rc(kh.at[(x + 2) % XD], rk, r_ss.at[0], r_rs.at[0], x_peer(1)),
                    rc(vh.at[(x + 2) % XD], rv, r_ss.at[1], r_rs.at[1], x_peer(3))]
        kv_send += kv_copies(1) + kv_copies(3)
        n_send = [rc(nh.at[(x + dd) % XD], nrecv.at[me_j], n_ss.at[i], n_rs.at[me_j], row_peer(dd, dc))
                  for i, (dd, dc) in enumerate(row_devs)]
        for cpy in kv_send + n_send:
            cpy.start()
        there = pl.ds((2 * 2 + c) * cache, cache)
        kv_relay = [rc(rk, kb.at[there], h_ss.at[0], k_rs.at[2 * 2 + c, 0], x_peer(1)),
                    rc(rv, vb.at[there], h_ss.at[1], k_rs.at[2 * 2 + c, 1], x_peer(3))]

        for dd in range(1, XD):
            src = (x + dd) % XD
            rc(qv.at[x], qx.at[src], q_ss.at[dd], q_rs.at[src], x_peer(dd)).wait_recv()

        def joined(pieces):
            return jnp.concatenate([v.astype(F32) for v in pieces], axis=0).astype(BF)

        qx[x] = qv[x]
        qall[pl.ds(0, UNIT), :] = joined([qx[i] for i in range(XD)])
        def half(w, h):
            start = w * UNIT + h * HALF
            return pl.ds(start if isinstance(w, int) else pl.multiple_of(start, 16), SIZE[h])

        b_send, late_send = (
            [rc(qall.at[half(0, h)], qall.at[half(w, h)], b_ss.at[2 * w + h], b_rs.at[2 * w + h], from_peer(w))
             for h in range(2) for w in ws] for ws in (straight, late))
        start_all(b_send)
        w_send = []
        for i, (hw, sy, sz, there_w) in enumerate(onward):
            w, h = hw // 2, hw % 2
            dev = at(x, (y + YD + sy) % YD, (z + ZD + sz) % ZD, c)
            w_send.append(rc(qall.at[half(w, h)], qall.at[half(there_w, h)], w_ss.at[i], b_rs.at[2 * there_w + h], dev))

        prefix = plen[0]
        riota = iota((256, 128), 0)
        lane0 = iota((256, 128), 1) == 0
        nblk = cache // 256

        def bias_block(b, _):
            slot = b // nblk
            base = ((row0 + (x + slot // 2) % XD) * 2 + slot % 2) * cache + (b % nblk) * 256
            hide = jnp.where(lane0 & (riota + base >= prefix), FILL, 0.0)
            bias[pl.ds(pl.multiple_of(b * 256, 256), 256), :] = hide.astype(BF)
            return 0

        lax.fori_loop(0, NCB, bias_block, 0)
        bias[pl.ds(NCB * 256, 256), :] = jnp.zeros((256, 128), BF)
        dev_j = lax.shift_right_logical(riota, 5)
        r_j = lax.bitwise_and(riota, PAD - 1)
        keyid[...] = jnp.where(r_j < tok, (row0 * 2 + dev_j) * tok + r_j, 1 << 23).astype(F32)

        r = (iota((NPAIR * 2, 256), 0) * 256 + iota((NPAIR * 2, 256), 1)).astype(F32)

        def parts(v, n):
            d = jnp.floor((v + 0.5) * (1.0 / n))
            return d, v - d * n

        unit_no, rest = parts(r, UNIT)
        chip_no, rest = parts(rest, PIECE)
        _, tok_no = parts(rest, tok)
        chip_row = jnp.zeros_like(r)
        for w, (dy, dz) in enumerate(offs):
            first_chip = ((z + dz) % ZD * YD + (y + dy) % YD) * XD
            chip_row = jnp.where(unit_no == w, first_chip.astype(F32), chip_row)
        tq[...] = ((chip_row + chip_no) * 2.0 + c.astype(F32)) * tok + tok_no

        def wait_half(hw, _):
            for h in range(2):
                @pl.when(hw % 2 == h)
                def _():
                    rc(qall.at[half(0, h)], qall.at[half(hw // 2, h)], b_ss.at[hw], b_rs.at[hw], mate).wait_recv()

            sends = {}
            for (k, *_), cpy in zip(onward, w_send):
                sends.setdefault(k, []).append(cpy)
            if sends:
                pl.when(hw <= max(sends))(lambda: on_value(
                    hw, {k: functools.partial(start_all, cpys) for k, cpys in sends.items()}))
            return 0

        def halves_for(p):
            last = p * 512 + 511
            n = last // UNIT * 2 + 1 + (last % UNIT >= HALF)
            return min(n, 2 * G) if isinstance(p, int) else jnp.minimum(n, 2 * G)

        def prep(p):
            for t in range(2):
                rows = qall[pl.ds(pl.multiple_of((p * 2 + t) * 256, 256), 256), :]
                qt[p * 2 + t] = rows.T

        ones_row = jnp.where(iota((128, 256), 0) == 0, 1.0, 0.0).astype(BF)

        def rep(v, n):
            return jnp.concatenate([v] * n, axis=0)

        def finish(p):
            for t in range(2):
                tile = p * 2 + t
                m = mraw[t]
                alpha = jnp.exp2((mb[tile] - m) * SCALE2)
                l = jnp.sum(lraw[t] + alpha * lb[tile], axis=0, keepdims=True)
                inv = 1.0 / l
                o = (oacc[tile] * rep(alpha, 16) + oraw[t]) * inv
                obuf[pl.ds(pl.multiple_of(tile * 256, 256), 256), :] = o.T.astype(BF)
                ls = m[0:1] * SCALE2 + jnp.log2(l)
                lbuf[tile * 2] = ls[:, 0:128]
                lbuf[tile * 2 + 1] = ls[:, 128:256]

        blocks_a = list(range(CHB))
        blocks_b = list(range(CHB, NKB))

        def unit_body(pv=None, pv_first=True, qk=None, qk_first=True, prep_pair=None, done_pair=None):
            pv_blocks = [] if pv is None else blocks_a if pv_first else blocks_b
            qk_blocks = [] if qk is None else blocks_a if qk_first else blocks_b
            if done_pair is not None:
                finish(done_pair)
            mp = [mcur[t] for t in range(2)]
            lacc = [jnp.zeros((8, 256), F32) for _ in range(2)]
            o = [None, None]
            mxs = [jnp.full((8, 256), -jnp.inf, F32) for _ in range(2)]

            def scores(b, t):
                k = jnp.concatenate([kb[pl.ds(b * 256, 256), :], bias[pl.ds(b * 256, 256), :]], axis=1)
                q = jnp.concatenate([qt[qk * 2 + t], ones_row], axis=0)
                return jnp.dot(k, q, preferred_element_type=F32)

            def keep(i, b, t, s):
                if b == NCB:
                    lim = tq[pl.ds(qk * 2 + t, 1), :]
                    kid = jnp.concatenate([keyid[...], keyid[...]], axis=1)
                    s = jnp.where(kid <= lim, s, FILL)
                sb[t, i] = s
                mxs[t] = jnp.maximum(mxs[t], s.reshape(32, 8, 256).max(0))

            def weigh(i, b, t):
                p = jnp.exp2((sb[t, i] - rep(mp[t], 32)) * SCALE2)
                lacc[t] = lacc[t] + p.reshape(32, 8, 256).sum(0)
                vt = jnp.concatenate([vb[pl.ds(b * 256, 128), :], vb[pl.ds(b * 256 + 128, 128), :]], axis=1)
                d = jnp.dot(vt, p.astype(BF), preferred_element_type=F32)
                o[t] = d if o[t] is None else o[t] + d

            for i in range(max(len(pv_blocks), len(qk_blocks))):
                for t in range(2):
                    if i < len(qk_blocks) and t == 0:
                        s = scores(qk_blocks[i], t)
                    if i < len(pv_blocks):
                        weigh(i, pv_blocks[i], t)
                    if i < len(qk_blocks):
                        keep(i, qk_blocks[i], t, s if t == 0 else scores(qk_blocks[i], t))
            if pv is not None:
                for t in range(2):
                    tile = pv * 2 + t
                    if pv_first:
                        oacc[tile] = o[t]
                        lb[tile] = lacc[t]
                    else:
                        oraw[t] = o[t]
                        lraw[t] = lacc[t]
                        mraw[t] = mp[t]
            if prep_pair is not None:
                prep(prep_pair)
            if qk is not None:
                for t in range(2):
                    m = jnp.broadcast_to(jnp.max(mxs[t], axis=0, keepdims=True), (8, 256))
                    if qk_first:
                        mb[qk * 2 + t] = m
                    else:
                        m = jnp.maximum(m, mb[qk * 2 + t])
                    mcur[t] = m

        def compute():
            other = pl.ds((1 - c) * cache, cache)
            for i, (src, dst) in enumerate(((kh, kb), (vh, vb))):
                rc(src.at[x], dst.at[other], k_ss.at[0, i], k_rs.at[1 - c, i], mate).wait_recv()
            prep(0)
            unit_body(qk=0)
            for hw in range(2, halves_for(min(1, NPAIR - 1))):
                wait_half(jnp.int32(hw), 0)
            prep(1)

            def forwarded(dx, cc):
                there = pl.ds((dx * 2 + cc) * cache, cache)
                return [rc(buf.at[there], buf.at[there], f_ss.at[dx, i], k_rs.at[dx * 2 + cc, i], mate)
                        for i, buf in enumerate((kb, vb))]

            def forward(dxs):
                for dx in dxs:
                    for cpy in forwarded(dx, c):
                        cpy.wait_recv()
                        cpy.start()

            def pass_a(u, _):
                lax.fori_loop(jnp.maximum(halves_for(u + 1), NEAR_END), jnp.maximum(halves_for(u + 2), NEAR_END), wait_half, 0)

                @pl.when(u == min(3, NPAIR - 2))
                def _():
                    for i, buf in enumerate((rk, rv)):
                        rc(buf, buf, r_ss.at[i], r_rs.at[i], mate).wait_recv()
                        kv_relay[i].start()

                @pl.when(u == min(14, NPAIR - 2))
                def _():
                    forward((1, 3))

                @pl.when(u == NPAIR - 2)
                def _():
                    forward((2,))

                unit_body(pv=u, qk=u + 1, prep_pair=jnp.minimum(u + 2, NPAIR - 1))
                return 0

            unit_body(pv=0, qk=1)
            lax.fori_loop(halves_for(1), max(halves_for(2), NEAR_END), wait_half, 0)
            start_all(late_send)
            prep(2)
            lax.fori_loop(1, NPAIR - 1, pass_a, 0)

            for i in range(1, 8):
                j = (me_j + i) % 8
                rc(nh.at[x], nrecv.at[j], n_ss.at[0], n_rs.at[j], mate).wait_recv()
            newv = jnp.concatenate([nrecv[j, 1] for j in range(8)], axis=0).T
            kb[pl.ds(NCB * 256, 256), :] = jnp.concatenate([nrecv[j, 0] for j in range(8)], axis=0)
            vb[pl.ds(NCB * 256, 128), :] = newv[:, 0:128]
            vb[pl.ds(NCB * 256 + 128, 128), :] = newv[:, 128:256]
            for dx in range(1, XD):
                for cpy in forwarded(dx, 1 - c):
                    cpy.wait_recv()
            unit_body(pv=NPAIR - 1, qk=NPAIR - 1, qk_first=False)

            def send_unit(p):
                done = {}
                for w in range(1, G):
                    for h in range(2):
                        done.setdefault((w * UNIT + h * HALF) // 512, []).extend(out_copies(w, h))
                on_value(p, {k: functools.partial(start_all, cpys) for k, cpys in done.items()})

            def pass_b(u, _):
                p = NPAIR - 1 - u
                unit_body(pv=p, pv_first=False, qk=p - 1, qk_first=False, done_pair=jnp.minimum(p + 1, NPAIR - 1))
                send_unit(p + 1)
                return 0

            lax.fori_loop(0, NPAIR - 1, pass_b, 0)
            finish(1)
            send_unit(jnp.int32(1))
            unit_body(pv=0, pv_first=False)
            finish(0)
            send_unit(jnp.int32(0))

        def out_copies(w, h):
            cpys = [rc(obuf.at[half(w, h)], orecv.at[w, half(0, h)], o_ss.at[2 * w + h], o_rs.at[2 * w + h], to_peer(w))]
            if h == 0:
                e0 = (w * UNIT) // 128
                cpys.append(rc(lbuf.at[pl.ds(e0, LSE_ROWS)], lrecv.at[w], l_ss.at[w], l_rs.at[w], to_peer(w)))
            return cpys

        compute()

        for w in range(1, G):
            for h in range(2):
                for cpy in out_copies(w, h):
                    cpy.wait_recv()
        lane = iota((LSE_ROWS, 128), 1)

        def shifted(v, off):
            if off == 0:
                return v
            r = pltpu.roll(v, 128 - off, 1)
            nxt = jnp.concatenate([r[1:], r[-1:]], axis=0)
            return jnp.where(lane[: v.shape[0]] < 128 - off, r, nxt)

        def lse_of(w):
            v = lbuf[pl.ds(0, LSE_ROWS)] if w == 0 else lrecv[w]
            return shifted(v.reshape(LSE_ROWS, 128), (w * UNIT) % 128)

        lses = [lse_of(w) for w in range(G)]
        top = functools.reduce(jnp.maximum, lses)
        wts = [jnp.exp2(v - top) for v in lses]
        den = functools.reduce(jnp.add, wts)
        inv = 1.0 / den
        wts = [v * inv for v in wts]
        total = (top + jnp.log2(den)) * LN2
        def bf(v):
            return v.astype(BF).astype(F32)

        cols = []
        for j in range(-(-UNIT // 128)):
            rows = jnp.concatenate([v[j:j + 1] for v in wts], axis=0)
            mid = rows - bf(rows)
            stack = [bf(rows), bf(mid), bf(mid - bf(mid)), jnp.zeros((128 - 3 * G, 128), F32)]
            cols.append(jnp.concatenate(stack, axis=0).T.astype(BF))
        cols = jnp.concatenate(cols, axis=0)[:UNIT]
        k0, k1 = iota((128, 256), 0), iota((128, 256), 1)
        final = jnp.zeros((UNIT, 128), F32)
        for w0 in range(0, G, 2):
            spread = jnp.where((k0 < 3 * G) & (k0 % G == w0 + lax.shift_right_logical(k1, 7)), 1.0, 0.0).astype(BF)
            lanes = jnp.dot(cols, spread, preferred_element_type=F32)
            for w in range(w0, min(w0 + 2, G)):
                src = obuf[pl.ds(0, UNIT), :] if w == 0 else orecv[w]
                final = final + src.astype(F32) * lanes[:, (w - w0) * 128:(w - w0 + 1) * 128]
        for i in range(XD):
            fo[i] = final[i * PIECE:(i + 1) * PIECE].astype(BF)
            off = (i * PIECE) % 128
            e = (i * PIECE) // 128
            need = min(3, LSE_ROWS - e)
            v = shifted(total[e:e + need], off)
            v = v if need >= 2 else jnp.concatenate([v, v], axis=0)
            fl[2 * i] = v[0:1]
            fl[2 * i + 1] = v[1:2]
        x_send = []
        for dd in range(1, XD):
            xd = (x + dd) % XD
            x_send.append(rc(fo.at[xd], out.at[x], x_ss.at[dd], x_rs.at[x], x_peer(dd)))
            x_send.append(rc(fl.at[pl.ds(2 * xd, 2)], flr.at[pl.ds(2 * x, 2)], y_ss.at[dd], y_rs.at[x], x_peer(dd)))
        for cpy in x_send:
            cpy.start()
        mine = pltpu.make_async_copy(fo.at[x], out.at[x], lsem.at[0])
        mine.start()
        flr[pl.ds(2 * x, 2)] = fl[pl.ds(2 * x, 2)]
        for dd in range(1, XD):
            src = (x + dd) % XD
            rc(fl.at[pl.ds(0, 2)], flr.at[pl.ds(2 * src, 2)], y_ss.at[dd], y_rs.at[src], x_peer(dd)).wait_recv()
        head_rows = []
        for i in range(KV):
            pair = flr[pl.ds(2 * i, 2)].reshape(2, 128)
            for g in range(RATIO):
                s = g * tok
                lo = pair[s // 128:s // 128 + 1]
                head_rows.append(lo if s % 128 == 0 else jnp.where(
                    lane[:1] < 128 - s % 128, pltpu.roll(lo, 128 - s % 128, 1), pltpu.roll(pair[1:2], 128 - s % 128, 1)))
        table = jnp.concatenate(head_rows + [jnp.zeros((32 - HEADS, 128), F32)], axis=0).T
        ltab[...] = table[:tok, :HEADS]
        lse_copy = pltpu.make_async_copy(ltab, lse_out, lsem.at[1])
        lse_copy.start()
        for cpy in q_send + kv_send + kv_relay + n_send + b_send + late_send + w_send + x_send:
            cpy.wait_send()
        for dx in range(1, XD):
            m = pl.ds((dx * 2 + c) * cache, cache)
            for i, buf in enumerate((kb, vb)):
                rc(buf.at[m], buf.at[m], f_ss.at[dx, i], k_rs.at[dx * 2 + c, i], mate).wait_send()
        for w in range(1, G):
            for cpy in out_copies(w, 0) + out_copies(w, 1):
                cpy.wait_send()
        for dd in range(1, XD):
            src = (x + dd) % XD
            rc(fo.at[0], out.at[src], x_ss.at[dd], x_rs.at[src], x_peer(dd)).wait_recv()
        mine.wait()
        lse_copy.wait()

    D, R = pltpu.SemaphoreType.DMA, NPAIR * 2
    V = pltpu.VMEM
    scratch = [
        V((XD, PIECE, 128), BF), V((cache * KV, 128), BF), V((cache * KV, 128), BF),
        V((tok * KV, 128), BF), V((tok * KV, 128), BF),
        V((KV, cache, 128), BF), V((KV, cache, 128), BF), V((KV, 2, PAD, 128), BF),
        V((cache, 128), BF), V((cache, 128), BF),
        V((NKB * 256, 128), BF), V((NKB * 256, 128), BF), V((NKB * 256, 128), BF),
        V((XD, PIECE, 128), BF),
        V((NPAIR * 512, 128), BF), V((R, 128, 256), BF),
        V((2, NKB - CHB, 256, 256), F32), V((R, 128, 256), F32),
        V((R, 8, 256), F32), V((R, 8, 256), F32), V((2, 8, 256), F32),
        V((2, 128, 256), F32), V((2, 8, 256), F32), V((2, 8, 256), F32), V((R, 256), F32),
        V((256, 128), F32), V((8, 2, PAD, 128), BF),
        V((NPAIR * 512, 128), BF), V((R * 2 + LSE_ROWS, 1, 128), F32),
        V((G, UNIT, 128), BF), V((G, LSE_ROWS, 1, 128), F32),
        V((XD, PIECE, 128), BF), V((2 * XD, 1, 128), F32), V((2 * XD, 1, 128), F32), V((tok, HEADS), F32),
        D((5,)), D((XD,)), D((XD,)), D((2 * G,)), D((2 * G,)), D((max(1, len(onward)),)),
        D((XD, 2)), D((2 * XD, 2)), D((XD, 2)), D((2,)), D((2,)), D((2,)), D((7,)), D((8,)),
        D((2 * G,)), D((2 * G,)), D((G,)), D((G,)), D((XD,)), D((XD,)), D((XD,)), D((XD,)),
    ]
    any_ = pl.BlockSpec(memory_space=pl.ANY)
    return pl.pallas_call(
        kernel,
        out_shape=(jax.ShapeDtypeStruct((XD, PIECE, 128), BF), jax.ShapeDtypeStruct((tok, HEADS), F32)),
        in_specs=[pl.BlockSpec(memory_space=pltpu.SMEM)] + [any_] * 5,
        out_specs=(any_, any_),
        scratch_shapes=scratch,
        name="prefix_attention",
        compiler_params=pltpu.CompilerParams(collective_id=0, has_side_effects=True, vmem_limit_bytes=63 << 20),
    )


def solution(mesh):
    spec = P(("dp", "cp"))

    def local(queries, key_new, value_new, key_cache, value_cache, prefix_len):
        tok, cache = queries.shape[0], key_cache.shape[0]
        call = make_kernel(tok, cache)
        q = queries.transpose(1, 0, 2).reshape(KV, RATIO * tok, HD)

        def rows(a):
            return a.reshape(a.shape[0] * KV, HD)

        out, row_lse = call(prefix_len, q, rows(key_cache), rows(value_cache), rows(key_new), rows(value_new))
        return out.reshape(HEADS, tok, HD).transpose(1, 0, 2), row_lse

    return jax.shard_map(local, mesh=mesh, in_specs=(spec,) * 5 + (P("dp"),), out_specs=(spec, spec), check_vma=False)
```

```python
import functools
import math

import jax
import jax.numpy as jnp
from jax import lax
from jax.experimental import pallas as pl
from jax.experimental.pallas import tpu as pltpu
from jax.sharding import PartitionSpec as P

ZD, YD, XD = 4, 4, 4

HEADS, KV, HD = 28, 4, 128
RATIO = HEADS // KV
FILL = -1e30
SCALE2 = HD ** -0.5 * math.log2(math.e)
LN2 = math.log(2.0)
PAD = 32
BF, F32 = jnp.bfloat16, jnp.float32


def ring_offsets():
    def hops(d, n):
        return min(d, n - d)

    offs = [(dy, dz) for dz in range(ZD) for dy in range(YD)]
    return sorted(offs, key=lambda o: (hops(o[0], YD) + hops(o[1], ZD), 0 in o, o[1], o[0]))


def on_value(v, actions):
    keys = sorted(actions)
    if len(keys) == 1:
        pl.when(v == keys[0])(actions[keys[0]])
    elif keys:
        mid = keys[len(keys) // 2]
        pl.when(v < mid)(lambda: on_value(v, {k: a for k, a in actions.items() if k < mid}))
        pl.when(v >= mid)(lambda: on_value(v, {k: a for k, a in actions.items() if k >= mid}))


def make_kernel(tok, cache):
    offs = ring_offsets()
    G = len(offs)
    PIECE = RATIO * tok
    UNIT = XD * PIECE
    ROWS = G * UNIT
    NPAIR = -(-ROWS // 512)
    CHB = 2 * cache // 256
    NCB = XD * CHB
    NKB = NCB + 1
    HALF = (UNIT // 2 + 31) // 32 * 32 if UNIT > 512 else UNIT // 2
    SIZE = (HALF, UNIT - HALF)
    assert HALF % 16 == 0 and UNIT % 16 == 0
    slot_of = {o: w for w, o in enumerate(offs)}
    straight = [w for w, o in enumerate(offs) if w and 0 in o and 2 not in o]
    late = [w for w, o in enumerate(offs) if o == (2, 2)]
    assert straight == list(range(1, len(straight) + 1))

    def toward(d, n):
        return 1 if d <= n // 2 else -1

    onward = []
    for w, (ty, tz) in enumerate(offs):
        if w == 0 or w in straight or w in late:
            continue
        if YD == 4 and ty == 2:
            via = [(1, 0), (-1, 0)]
        elif ZD == 4 and tz == 2:
            via = [(0, 1), (0, -1)]
        else:
            via = [(toward(ty, YD), 0), (0, toward(tz, ZD))]
        for h, (ny, nz) in enumerate(via):
            onward.append((2 * slot_of[(ty - ny) % YD, (tz - nz) % ZD] + h, -ny, -nz, w))
    onward.sort()
    NEAR_END = 2 * (len(straight) + 1)
    LSE_ROWS = UNIT // 128 + 1
    assert cache % 256 == 0 and 8 * PAD == 256 and tok <= PAD

    def kernel(plen, q_in, k_in, v_in, kn_in, vn_in, out, lse_out,
               qv, kraw, vraw, knraw, vnraw, kh, vh, nh, rk, rv,
               kb, vb, bias, qx, qall, qt, sb, oacc, mb, lb, mcur, oraw, lraw, mraw, tq, keyid, nrecv,
               obuf, lbuf, orecv, lrecv, fo, fl,
               lsem, q_ss, q_rs, b_ss, b_rs, w_ss, k_ss, k_rs, f_ss, r_ss, r_rs, h_ss, n_ss, n_rs,
               o_ss, o_rs, l_ss, l_rs, x_ss, x_rs, y_ss, y_rs):
        cp = lax.axis_index("cp")
        c = cp % 2
        x = (cp // 2) % XD
        y = (cp // (2 * XD)) % YD
        z = cp // (2 * XD * YD)
        row0 = (z * YD + y) * XD

        def at(xx, yy, zz, cc):
            return ((zz * YD + yy) * XD + xx) * 2 + cc

        def x_peer(dd):
            return at((x + dd) % XD, y, z, c)

        mate = at(x, y, z, 1 - c)

        def to_peer(w):
            dy, dz = offs[w]
            return at(x, (y + dy) % YD, (z + dz) % ZD, c)

        def from_peer(w):
            dy, dz = offs[w]
            return at(x, (y + YD - dy) % YD, (z + ZD - dz) % ZD, c)

        def start_all(cpys):
            for cpy in cpys:
                cpy.start()

        def rc(src, dst, ss, rs, dev):
            return pltpu.make_async_remote_copy(
                src_ref=src, dst_ref=dst, send_sem=ss, recv_sem=rs,
                device_id={"cp": dev}, device_id_type=pl.DeviceIdType.MESH)

        row_devs = [(dd, dc) for dd in range(XD) for dc in range(2) if (dd, dc) != (0, 0)]

        def row_peer(dd, dc):
            return at((x + dd) % XD, y, z, (c + dc) % 2)

        barrier = pltpu.get_barrier_semaphore()
        peers = [to_peer(w) for w in range(1, G)] + [row_peer(dd, dc) for dd, dc in row_devs]
        for p in peers:
            pl.semaphore_signal(barrier, inc=1, device_id={"cp": p}, device_id_type=pl.DeviceIdType.MESH)
        me_j = x * 2 + c
        own = pl.ds(c * cache, cache)
        local = [pltpu.make_async_copy(src, dst, lsem.at[i]) for i, (src, dst) in enumerate(
            [(q_in, qv), (k_in, kraw), (v_in, vraw), (kn_in, knraw), (vn_in, vnraw)])]
        for cpy in local:
            cpy.start()
        local[0].wait()
        pl.semaphore_wait(barrier, len(peers))

        q_send = [rc(qv.at[(x + dd) % XD], qx.at[x], q_ss.at[dd], q_rs.at[x], x_peer(dd)) for dd in (2, 1, 3)]
        start_all(q_send)

        def iota(shape, d):
            return lax.broadcasted_iota(jnp.int32, shape, d)

        i0, i1 = iota((256, 256), 0), iota((256, 256), 1)
        pick = jnp.where(i1 == (i0 & 63) * KV + lax.shift_right_logical(i0, 6), 1.0, 0.0).astype(BF)
        for cpy in local[1:]:
            cpy.wait()
        groups = cache // 128
        unroll = max(u for u in (1, 2, 4) if groups % u == 0)

        def split(g0, _):
            for du in range(unroll):
                g = g0 * unroll + du
                for raw, dst, flip in ((kraw, kh, False), (vraw, vh, True)):
                    rows = raw[pl.ds(pl.multiple_of(g * 128 * KV, 256), 128 * KV), :]
                    both = jnp.concatenate([rows[:256], rows[256:]], axis=1)
                    r = jnp.dot(pick, both, preferred_element_type=F32).astype(BF)
                    for h in range(KV):
                        one = jnp.concatenate([r[h * 64:(h + 1) * 64, :128], r[h * 64:(h + 1) * 64, 128:]], axis=0)
                        dst[h, pl.ds(pl.multiple_of(g * 128, 128), 128), :] = one.T if flip else one
            return 0

        lax.fori_loop(0, groups // unroll, split, 0)
        kb[own, :] = kh[x]
        vb[own, :] = vh[x]
        n0, n1 = iota((KV * PAD, tok * KV), 0), iota((KV * PAD, tok * KV), 1)
        npick = jnp.where((n0 % PAD < tok) & (n1 == (n0 % PAD) * KV + n0 // PAD), 1.0, 0.0).astype(BF)
        for i, raw in enumerate((knraw, vnraw)):
            r = jnp.dot(npick, raw[...], preferred_element_type=F32).astype(BF)
            for h in range(KV):
                nh[h, i] = r[h * PAD:(h + 1) * PAD]
        nrecv[me_j] = nh[x]

        def kv_copies(dd):
            slot = ((XD - dd) % XD) * 2 + c
            there = pl.ds(slot * cache, cache)
            dev = x_peer(dd) if dd else mate
            return [rc(src.at[(x + dd) % XD], dst.at[there], k_ss.at[dd, i], k_rs.at[slot, i], dev)
                    for i, (src, dst) in enumerate(((kh, kb), (vh, vb)))]

        kv_send = kv_copies(0)
        kv_send += [rc(kh.at[(x + 2) % XD], rk, r_ss.at[0], r_rs.at[0], x_peer(1)),
                    rc(vh.at[(x + 2) % XD], rv, r_ss.at[1], r_rs.at[1], x_peer(3))]
        kv_send += kv_copies(1) + kv_copies(3)
        n_send = [rc(nh.at[(x + dd) % XD], nrecv.at[me_j], n_ss.at[i], n_rs.at[me_j], row_peer(dd, dc))
                  for i, (dd, dc) in enumerate(row_devs)]
        for cpy in kv_send + n_send:
            cpy.start()
        there = pl.ds((2 * 2 + c) * cache, cache)
        kv_relay = [rc(rk, kb.at[there], h_ss.at[0], k_rs.at[2 * 2 + c, 0], x_peer(1)),
                    rc(rv, vb.at[there], h_ss.at[1], k_rs.at[2 * 2 + c, 1], x_peer(3))]

        for dd in range(1, XD):
            src = (x + dd) % XD
            rc(qv.at[x], qx.at[src], q_ss.at[dd], q_rs.at[src], x_peer(dd)).wait_recv()

        def joined(pieces):
            return jnp.concatenate([v.astype(F32) for v in pieces], axis=0).astype(BF)

        qx[x] = qv[x]
        qall[pl.ds(0, UNIT), :] = joined([qx[i] for i in range(XD)])
        def half(w, h):
            start = w * UNIT + h * HALF
            return pl.ds(start if isinstance(w, int) else pl.multiple_of(start, 16), SIZE[h])

        b_send, late_send = (
            [rc(qall.at[half(0, h)], qall.at[half(w, h)], b_ss.at[2 * w + h], b_rs.at[2 * w + h], from_peer(w))
             for h in range(2) for w in ws] for ws in (straight, late))
        start_all(b_send)
        w_send = []
        for i, (hw, sy, sz, there_w) in enumerate(onward):
            w, h = hw // 2, hw % 2
            dev = at(x, (y + YD + sy) % YD, (z + ZD + sz) % ZD, c)
            w_send.append(rc(qall.at[half(w, h)], qall.at[half(there_w, h)], w_ss.at[i], b_rs.at[2 * there_w + h], dev))

        prefix = plen[0]
        riota = iota((256, 128), 0)
        lane0 = iota((256, 128), 1) == 0
        nblk = cache // 256

        def bias_block(b, _):
            slot = b // nblk
            base = ((row0 + (x + slot // 2) % XD) * 2 + slot % 2) * cache + (b % nblk) * 256
            hide = jnp.where(lane0 & (riota + base >= prefix), FILL, 0.0)
            bias[pl.ds(pl.multiple_of(b * 256, 256), 256), :] = hide.astype(BF)
            return 0

        lax.fori_loop(0, NCB, bias_block, 0)
        bias[pl.ds(NCB * 256, 256), :] = jnp.zeros((256, 128), BF)
        dev_j = lax.shift_right_logical(riota, 5)
        r_j = lax.bitwise_and(riota, PAD - 1)
        keyid[...] = jnp.where(r_j < tok, (row0 * 2 + dev_j) * tok + r_j, 1 << 23).astype(F32)

        r = (iota((NPAIR * 2, 256), 0) * 256 + iota((NPAIR * 2, 256), 1)).astype(F32)

        def parts(v, n):
            d = jnp.floor((v + 0.5) * (1.0 / n))
            return d, v - d * n

        unit_no, rest = parts(r, UNIT)
        chip_no, rest = parts(rest, PIECE)
        _, tok_no = parts(rest, tok)
        chip_row = jnp.zeros_like(r)
        for w, (dy, dz) in enumerate(offs):
            first_chip = ((z + dz) % ZD * YD + (y + dy) % YD) * XD
            chip_row = jnp.where(unit_no == w, first_chip.astype(F32), chip_row)
        tq[...] = ((chip_row + chip_no) * 2.0 + c.astype(F32)) * tok + tok_no

        def arrived(w, h):
            rc(qall.at[half(0, h)], qall.at[half(w, h)], b_ss.at[2 * w + h], b_rs.at[2 * w + h], mate).wait_recv()

        def wait_near(hw):
            arrived(hw // 2, hw % 2)
            for (k, *_), cpy in zip(onward, w_send):
                if k == hw:
                    cpy.start()

        def wait_far(w):
            for h in range(2):
                arrived(w, h)
            relays = {}
            for (k, *_), cpy in zip(onward, w_send):
                if k >= NEAR_END:
                    relays.setdefault(k // 2, []).append(cpy)
            if relays:
                pl.when(w <= max(relays))(lambda: on_value(
                    w, {k: functools.partial(start_all, cpys) for k, cpys in relays.items()}))

        def halves_for(p):
            last = p * 512 + 511
            n = last // UNIT * 2 + 1 + (last % UNIT >= HALF)
            return min(n, 2 * G)

        def units_for(p):
            return jnp.clip((p * 512 + 511) // UNIT + 1, len(straight) + 1, G)

        def prep(p):
            for t in range(2):
                rows = qall[pl.ds(pl.multiple_of((p * 2 + t) * 256, 256), 256), :]
                qt[p * 2 + t] = rows.T

        ones_row = jnp.where(iota((128, 256), 0) == 0, 1.0, 0.0).astype(BF)

        def rep(v, n):
            return jnp.concatenate([v] * n, axis=0)

        def finish(p):
            for t in range(2):
                tile = p * 2 + t
                m = mraw[t]
                alpha = jnp.exp2((mb[tile] - m) * SCALE2)
                l = jnp.sum(lraw[t] + alpha * lb[tile], axis=0, keepdims=True)
                inv = 1.0 / l
                o = (oacc[tile] * rep(alpha, 16) + oraw[t]) * inv
                obuf[pl.ds(pl.multiple_of(tile * 256, 256), 256), :] = o.T.astype(BF)
                ls = m[0:1] * SCALE2 + jnp.log2(l)
                lbuf[tile * 2] = ls[:, 0:128]
                lbuf[tile * 2 + 1] = ls[:, 128:256]

        blocks_a = list(range(CHB))
        blocks_b = list(range(CHB, NKB))

        def unit_body(pv=None, pv_first=True, qk=None, qk_first=True, prep_pair=None, done_pair=None):
            pv_blocks = [] if pv is None else blocks_a if pv_first else blocks_b
            qk_blocks = [] if qk is None else blocks_a if qk_first else blocks_b
            if done_pair is not None:
                finish(done_pair)
            mp = [mcur[t] for t in range(2)]
            lacc = [jnp.zeros((8, 256), F32) for _ in range(2)]
            o = [None, None]
            mxs = [jnp.full((8, 256), -jnp.inf, F32) for _ in range(2)]

            def scores(b, t):
                k = jnp.concatenate([kb[pl.ds(b * 256, 256), :], bias[pl.ds(b * 256, 256), :]], axis=1)
                q = jnp.concatenate([qt[qk * 2 + t], ones_row], axis=0)
                return jnp.dot(k, q, preferred_element_type=F32)

            def keep(i, b, t, s):
                if b == NCB:
                    lim = tq[pl.ds(qk * 2 + t, 1), :]
                    kid = jnp.concatenate([keyid[...], keyid[...]], axis=1)
                    s = jnp.where(kid <= lim, s, FILL)
                sb[t, i] = s
                mxs[t] = jnp.maximum(mxs[t], s.reshape(32, 8, 256).max(0))

            def weigh(i, b, t):
                p = jnp.exp2((sb[t, i] - rep(mp[t], 32)) * SCALE2)
                lacc[t] = lacc[t] + p.reshape(32, 8, 256).sum(0)
                vt = jnp.concatenate([vb[pl.ds(b * 256, 128), :], vb[pl.ds(b * 256 + 128, 128), :]], axis=1)
                d = jnp.dot(vt, p.astype(BF), preferred_element_type=F32)
                o[t] = d if o[t] is None else o[t] + d

            for i in range(max(len(pv_blocks), len(qk_blocks))):
                for t in range(2):
                    if i < len(qk_blocks) and t == 0:
                        s = scores(qk_blocks[i], t)
                    if i < len(pv_blocks):
                        weigh(i, pv_blocks[i], t)
                    if i < len(qk_blocks):
                        keep(i, qk_blocks[i], t, s if t == 0 else scores(qk_blocks[i], t))
            if pv is not None:
                for t in range(2):
                    tile = pv * 2 + t
                    if pv_first:
                        oacc[tile] = o[t]
                        lb[tile] = lacc[t]
                    else:
                        oraw[t] = o[t]
                        lraw[t] = lacc[t]
                        mraw[t] = mp[t]
            if prep_pair is not None:
                prep(prep_pair)
            if qk is not None:
                for t in range(2):
                    m = jnp.broadcast_to(jnp.max(mxs[t], axis=0, keepdims=True), (8, 256))
                    if qk_first:
                        mb[qk * 2 + t] = m
                    else:
                        m = jnp.maximum(m, mb[qk * 2 + t])
                    mcur[t] = m

        def compute():
            other = pl.ds((1 - c) * cache, cache)
            for i, (src, dst) in enumerate(((kh, kb), (vh, vb))):
                rc(src.at[x], dst.at[other], k_ss.at[0, i], k_rs.at[1 - c, i], mate).wait_recv()
            prep(0)
            unit_body(qk=0)
            first_end = halves_for(min(1, NPAIR - 1))
            for hw in range(2, first_end):
                wait_near(hw)
            prep(1)

            def forwarded(dx, cc):
                there = pl.ds((dx * 2 + cc) * cache, cache)
                return [rc(buf.at[there], buf.at[there], f_ss.at[dx, i], k_rs.at[dx * 2 + cc, i], mate)
                        for i, buf in enumerate((kb, vb))]

            def forward(dxs):
                for dx in dxs:
                    for cpy in forwarded(dx, c):
                        cpy.wait_recv()
                        cpy.start()

            def pass_a(u, _):
                have, need = units_for(u + 1), units_for(u + 2)
                pl.when(need > have)(lambda: wait_far(have))

                @pl.when(u == min(3, NPAIR - 2))
                def _():
                    for i, buf in enumerate((rk, rv)):
                        rc(buf, buf, r_ss.at[i], r_rs.at[i], mate).wait_recv()
                        kv_relay[i].start()

                @pl.when(u == min(14, NPAIR - 2))
                def _():
                    forward((1, 3))

                @pl.when(u == NPAIR - 2)
                def _():
                    forward((2,))

                unit_body(pv=u, qk=u + 1, prep_pair=jnp.minimum(u + 2, NPAIR - 1))
                return 0

            unit_body(pv=0, qk=1)
            for hw in range(first_end, NEAR_END):
                wait_near(hw)
            start_all(late_send)
            for w in range(len(straight) + 1, (halves_for(2) + 1) // 2):
                wait_far(jnp.int32(w))
            prep(2)
            lax.fori_loop(1, NPAIR - 1, pass_a, 0)

            for i in range(1, 8):
                j = (me_j + i) % 8
                rc(nh.at[x], nrecv.at[j], n_ss.at[0], n_rs.at[j], mate).wait_recv()
            newv = jnp.concatenate([nrecv[j, 1] for j in range(8)], axis=0).T
            kb[pl.ds(NCB * 256, 256), :] = jnp.concatenate([nrecv[j, 0] for j in range(8)], axis=0)
            vb[pl.ds(NCB * 256, 128), :] = newv[:, 0:128]
            vb[pl.ds(NCB * 256 + 128, 128), :] = newv[:, 128:256]
            for dx in range(1, XD):
                for cpy in forwarded(dx, 1 - c):
                    cpy.wait_recv()
            unit_body(pv=NPAIR - 1, qk=NPAIR - 1, qk_first=False)

            def copies_done(pairs):
                return [cpy for w in range(1, G) for h in range(2) if (w * UNIT + h * HALF) // 512 in pairs
                        for cpy in out_copies(w, h)]

            leave, prev = {}, NPAIR
            for u in sorted({NPAIR - 2 - d for d in (0, 1, 2, 4, 6, 9, 13, 17) if NPAIR - 2 - d >= 1}):
                leave[u] = functools.partial(start_all, copies_done(range(NPAIR - u, prev)))
                prev = NPAIR - u

            def pass_b(u, _):
                p = NPAIR - 1 - u
                unit_body(pv=p, pv_first=False, qk=p - 1, qk_first=False, done_pair=jnp.minimum(p + 1, NPAIR - 1))
                on_value(u, leave)
                return 0

            lax.fori_loop(0, NPAIR - 1, pass_b, 0)
            finish(1)
            start_all(copies_done(range(1, prev)))
            unit_body(pv=0, pv_first=False)
            finish(0)
            start_all(copies_done([0]))

        def out_copies(w, h):
            cpys = [rc(obuf.at[half(w, h)], orecv.at[w, half(0, h)], o_ss.at[2 * w + h], o_rs.at[2 * w + h], to_peer(w))]
            if h == 0:
                e0 = (w * UNIT) // 128
                cpys.append(rc(lbuf.at[pl.ds(e0, LSE_ROWS)], lrecv.at[w], l_ss.at[w], l_rs.at[w], to_peer(w)))
            return cpys

        compute()

        for w in range(1, G):
            for h in range(2):
                for cpy in out_copies(w, h):
                    cpy.wait_recv()
        lane = iota((LSE_ROWS, 128), 1)

        def shifted(v, off):
            if off == 0:
                return v
            r = pltpu.roll(v, 128 - off, 1)
            nxt = jnp.concatenate([r[1:], r[-1:]], axis=0)
            return jnp.where(lane[: v.shape[0]] < 128 - off, r, nxt)

        def lse_of(w):
            v = lbuf[pl.ds(0, LSE_ROWS)] if w == 0 else lrecv[w]
            return shifted(v.reshape(LSE_ROWS, 128), (w * UNIT) % 128)

        lses = [lse_of(w) for w in range(G)]
        top = functools.reduce(jnp.maximum, lses)
        wts = [jnp.exp2(v - top) for v in lses]
        den = functools.reduce(jnp.add, wts)
        inv = 1.0 / den
        wts = [v * inv for v in wts]
        total = (top + jnp.log2(den)) * LN2
        def bf(v):
            return v.astype(BF).astype(F32)

        cols = []
        for j in range(-(-UNIT // 128)):
            rows = jnp.concatenate([v[j:j + 1] for v in wts], axis=0)
            mid = rows - bf(rows)
            stack = [bf(rows), bf(mid), bf(mid - bf(mid)), jnp.zeros((128 - 3 * G, 128), F32)]
            cols.append(jnp.concatenate(stack, axis=0).T.astype(BF))
        cols = jnp.concatenate(cols, axis=0)[:UNIT]
        k0, k1 = iota((128, 256), 0), iota((128, 256), 1)
        final = jnp.zeros((UNIT, 128), F32)
        for w0 in range(0, G, 2):
            spread = jnp.where((k0 < 3 * G) & (k0 % G == w0 + lax.shift_right_logical(k1, 7)), 1.0, 0.0).astype(BF)
            lanes = jnp.dot(cols, spread, preferred_element_type=F32)
            for w in range(w0, min(w0 + 2, G)):
                src = obuf[pl.ds(0, UNIT), :] if w == 0 else orecv[w]
                final = final + src.astype(F32) * lanes[:, (w - w0) * 128:(w - w0 + 1) * 128]
        for i in range(XD):
            fo[i] = final[i * PIECE:(i + 1) * PIECE].astype(BF)
            off = (i * PIECE) % 128
            e = (i * PIECE) // 128
            need = min(3, LSE_ROWS - e)
            v = shifted(total[e:e + need], off)
            v = v if need >= 2 else jnp.concatenate([v, v], axis=0)
            fl[2 * i] = v[0:1]
            fl[2 * i + 1] = v[1:2]
        x_send = []
        for dd in range(1, XD):
            xd = (x + dd) % XD
            x_send.append(rc(fo.at[xd], out.at[x], x_ss.at[dd], x_rs.at[x], x_peer(dd)))
            x_send.append(rc(fl.at[pl.ds(2 * xd, 2)], lse_out.at[pl.ds(2 * x, 2)], y_ss.at[dd], y_rs.at[x], x_peer(dd)))
        for cpy in x_send:
            cpy.start()
        mine = pltpu.make_async_copy(fo.at[x], out.at[x], lsem.at[0])
        mine.start()
        lse_copy = pltpu.make_async_copy(fl.at[pl.ds(2 * x, 2)], lse_out.at[pl.ds(2 * x, 2)], lsem.at[1])
        lse_copy.start()
        for dd in range(1, XD):
            src = (x + dd) % XD
            rc(fl.at[pl.ds(0, 2)], lse_out.at[pl.ds(2 * src, 2)], y_ss.at[dd], y_rs.at[src], x_peer(dd)).wait_recv()
        for cpy in q_send + kv_send + kv_relay + n_send + b_send + late_send + w_send + x_send:
            cpy.wait_send()
        for dx in range(1, XD):
            m = pl.ds((dx * 2 + c) * cache, cache)
            for i, buf in enumerate((kb, vb)):
                rc(buf.at[m], buf.at[m], f_ss.at[dx, i], k_rs.at[dx * 2 + c, i], mate).wait_send()
        for w in range(1, G):
            for cpy in out_copies(w, 0) + out_copies(w, 1):
                cpy.wait_send()
        for dd in range(1, XD):
            src = (x + dd) % XD
            rc(fo.at[0], out.at[src], x_ss.at[dd], x_rs.at[src], x_peer(dd)).wait_recv()
        mine.wait()
        lse_copy.wait()

    D, R = pltpu.SemaphoreType.DMA, NPAIR * 2
    V = pltpu.VMEM
    scratch = [
        V((XD, PIECE, 128), BF), V((cache * KV, 128), BF), V((cache * KV, 128), BF),
        V((tok * KV, 128), BF), V((tok * KV, 128), BF),
        V((KV, cache, 128), BF), V((KV, cache, 128), BF), V((KV, 2, PAD, 128), BF),
        V((cache, 128), BF), V((cache, 128), BF),
        V((NKB * 256, 128), BF), V((NKB * 256, 128), BF), V((NKB * 256, 128), BF),
        V((XD, PIECE, 128), BF),
        V((NPAIR * 512, 128), BF), V((R, 128, 256), BF),
        V((2, NKB - CHB, 256, 256), F32), V((R, 128, 256), F32),
        V((R, 8, 256), F32), V((R, 8, 256), F32), V((2, 8, 256), F32),
        V((2, 128, 256), F32), V((2, 8, 256), F32), V((2, 8, 256), F32), V((R, 256), F32),
        V((256, 128), F32), V((8, 2, PAD, 128), BF),
        V((NPAIR * 512, 128), BF), V((R * 2 + LSE_ROWS, 1, 128), F32),
        V((G, UNIT, 128), BF), V((G, LSE_ROWS, 1, 128), F32),
        V((XD, PIECE, 128), BF), V((2 * XD, 1, 128), F32),
        D((5,)), D((XD,)), D((XD,)), D((2 * G,)), D((2 * G,)), D((max(1, len(onward)),)),
        D((XD, 2)), D((2 * XD, 2)), D((XD, 2)), D((2,)), D((2,)), D((2,)), D((7,)), D((8,)),
        D((2 * G,)), D((2 * G,)), D((G,)), D((G,)), D((XD,)), D((XD,)), D((XD,)), D((XD,)),
    ]
    any_ = pl.BlockSpec(memory_space=pl.ANY)
    return pl.pallas_call(
        kernel,
        out_shape=(jax.ShapeDtypeStruct((XD, PIECE, 128), BF), jax.ShapeDtypeStruct((2 * XD, 1, 128), F32)),
        in_specs=[pl.BlockSpec(memory_space=pltpu.SMEM)] + [any_] * 5,
        out_specs=(any_, any_),
        scratch_shapes=scratch,
        name="prefix_attention",
        compiler_params=pltpu.CompilerParams(collective_id=0, has_side_effects=True, vmem_limit_bytes=63 << 20),
    )


def make_finish(tok):
    rows = RATIO * tok

    def kernel(o_in, l_in, o_out, l_out, o_buf, l_buf, table, sem):
        o_get = pltpu.make_async_copy(o_in, o_buf, sem.at[0])
        l_get = pltpu.make_async_copy(l_in, l_buf, sem.at[1])
        o_get.start()
        l_get.start()
        l_get.wait()
        lane = lax.broadcasted_iota(jnp.int32, (1, 128), 1)
        head_rows = []
        for i in range(KV):
            pair = l_buf[pl.ds(2 * i, 2)].reshape(2, 128)
            for g in range(RATIO):
                s = g * tok
                lo, back = pair[s // 128:s // 128 + 1], 128 - s % 128
                head_rows.append(lo if back == 128 else jnp.where(
                    lane < back, pltpu.roll(lo, back, 1), pltpu.roll(pair[1:2], back, 1)))
        table[...] = jnp.concatenate(head_rows + [jnp.zeros((32 - HEADS, 128), F32)], axis=0).T[:tok, :HEADS]
        l_put = pltpu.make_async_copy(table, l_out, sem.at[2])
        l_put.start()
        o_get.wait()
        o_put = pltpu.make_async_copy(o_buf, o_out, sem.at[3])
        o_put.start()
        l_put.wait()
        o_put.wait()

    V, any_ = pltpu.VMEM, pl.BlockSpec(memory_space=pl.ANY)
    return pl.pallas_call(
        kernel,
        out_shape=(jax.ShapeDtypeStruct((KV, rows, HD), BF), jax.ShapeDtypeStruct((tok, HEADS), F32)),
        in_specs=[any_, any_],
        out_specs=(any_, any_),
        scratch_shapes=[V((KV, rows, HD), BF), V((2 * KV, 1, 128), F32), V((tok, HEADS), F32),
                        pltpu.SemaphoreType.DMA((4,))],
        name="final_form",
    )


def solution(mesh):
    spec = P(("dp", "cp"))

    def local(queries, key_new, value_new, key_cache, value_cache, prefix_len):
        tok, cache = queries.shape[0], key_cache.shape[0]
        call = make_kernel(tok, cache)
        q = queries.transpose(1, 0, 2).reshape(KV, RATIO * tok, HD)

        def rows(a):
            return a.reshape(a.shape[0] * KV, HD)

        out, row_lse = make_finish(tok)(*call(prefix_len, q, rows(key_cache), rows(value_cache), rows(key_new), rows(value_new)))
        return out.reshape(HEADS, tok, HD).transpose(1, 0, 2), row_lse

    return jax.shard_map(local, mesh=mesh, in_specs=(spec,) * 5 + (P("dp"),), out_specs=(spec, spec), check_vma=False)
```

```python
import functools
import math

import jax
import jax.numpy as jnp
from jax import lax
from jax.experimental import pallas as pl
from jax.experimental.pallas import tpu as pltpu
from jax.sharding import PartitionSpec as P

ZD, YD, XD = 4, 4, 4

HEADS, KV, HD = 28, 4, 128
RATIO = HEADS // KV
FILL = -1e30
SCALE2 = HD ** -0.5 * math.log2(math.e)
LN2 = math.log(2.0)
PAD = 32
BF, F32 = jnp.bfloat16, jnp.float32


def ring_offsets():
    def hops(d, n):
        return min(d, n - d)

    offs = [(dy, dz) for dz in range(ZD) for dy in range(YD)]
    return sorted(offs, key=lambda o: (hops(o[0], YD) + hops(o[1], ZD), 0 in o, o[1], o[0]))


def on_value(v, actions):
    keys = sorted(actions)
    if len(keys) == 1:
        pl.when(v == keys[0])(actions[keys[0]])
    elif keys:
        mid = keys[len(keys) // 2]
        pl.when(v < mid)(lambda: on_value(v, {k: a for k, a in actions.items() if k < mid}))
        pl.when(v >= mid)(lambda: on_value(v, {k: a for k, a in actions.items() if k >= mid}))


def make_kernel(tok, cache):
    offs = ring_offsets()
    G = len(offs)
    PIECE = RATIO * tok
    UNIT = XD * PIECE
    ROWS = G * UNIT
    NPAIR = -(-ROWS // 512)
    CHB = 2 * cache // 256
    NCB = XD * CHB
    NKB = NCB + 1
    HALF = (UNIT // 2 + 31) // 32 * 32 if UNIT > 512 else UNIT // 2
    SIZE = (HALF, UNIT - HALF)
    assert HALF % 16 == 0 and UNIT % 16 == 0
    slot_of = {o: w for w, o in enumerate(offs)}
    straight = [w for w, o in enumerate(offs) if w and 0 in o and 2 not in o]
    late = [w for w, o in enumerate(offs) if o == (2, 2)]
    assert straight == list(range(1, len(straight) + 1))

    def toward(d, n):
        return 1 if d <= n // 2 else -1

    onward = []
    for w, (ty, tz) in enumerate(offs):
        if w == 0 or w in straight or w in late:
            continue
        if YD == 4 and ty == 2:
            via = [(1, 0), (-1, 0)]
        elif ZD == 4 and tz == 2:
            via = [(0, 1), (0, -1)]
        else:
            via = [(toward(ty, YD), 0), (0, toward(tz, ZD))]
        for h, (ny, nz) in enumerate(via):
            onward.append((2 * slot_of[(ty - ny) % YD, (tz - nz) % ZD] + h, -ny, -nz, w))
    onward.sort()
    NEAR_END = 2 * (len(straight) + 1)
    LSE_ROWS = UNIT // 128 + 1
    assert cache % 256 == 0 and 8 * PAD == 256 and tok <= PAD

    def kernel(plen, q_in, k_in, v_in, kn_in, vn_in, out, lse_out,
               qv, kraw, vraw, knraw, vnraw, kh, vh, nh, rk, rv,
               kb, vb, bias, qx, qall, qt, sb, oacc, mb, lb, mcur, oraw, lraw, mraw, tq, keyid, nrecv,
               obuf, lbuf, orecv, lrecv, fo, fl,
               lsem, q_ss, q_rs, b_ss, b_rs, w_ss, k_ss, k_rs, f_ss, r_ss, r_rs, h_ss, n_ss, n_rs,
               o_ss, o_rs, l_ss, l_rs, x_ss, x_rs, y_ss, y_rs):
        cp = lax.axis_index("cp")
        c = cp % 2
        x = (cp // 2) % XD
        y = (cp // (2 * XD)) % YD
        z = cp // (2 * XD * YD)
        row0 = (z * YD + y) * XD

        def at(xx, yy, zz, cc):
            return ((zz * YD + yy) * XD + xx) * 2 + cc

        def x_peer(dd):
            return at((x + dd) % XD, y, z, c)

        mate = at(x, y, z, 1 - c)

        def to_peer(w):
            dy, dz = offs[w]
            return at(x, (y + dy) % YD, (z + dz) % ZD, c)

        def from_peer(w):
            dy, dz = offs[w]
            return at(x, (y + YD - dy) % YD, (z + ZD - dz) % ZD, c)

        def start_all(cpys):
            for cpy in cpys:
                cpy.start()

        def rc(src, dst, ss, rs, dev):
            return pltpu.make_async_remote_copy(
                src_ref=src, dst_ref=dst, send_sem=ss, recv_sem=rs,
                device_id={"cp": dev}, device_id_type=pl.DeviceIdType.MESH)

        row_devs = [(dd, dc) for dd in range(XD) for dc in range(2) if (dd, dc) != (0, 0)]

        def row_peer(dd, dc):
            return at((x + dd) % XD, y, z, (c + dc) % 2)

        barrier = pltpu.get_barrier_semaphore()
        peers = [to_peer(w) for w in range(1, G)] + [row_peer(dd, dc) for dd, dc in row_devs]
        for p in peers:
            pl.semaphore_signal(barrier, inc=1, device_id={"cp": p}, device_id_type=pl.DeviceIdType.MESH)
        me_j = x * 2 + c
        own = pl.ds(c * cache, cache)
        local = [pltpu.make_async_copy(src, dst, lsem.at[i]) for i, (src, dst) in enumerate(
            [(q_in, qv), (k_in, kraw), (v_in, vraw), (kn_in, knraw), (vn_in, vnraw)])]
        for cpy in local:
            cpy.start()
        local[0].wait()
        pl.semaphore_wait(barrier, len(peers))

        q_send = [rc(qv.at[(x + dd) % XD], qx.at[x], q_ss.at[dd], q_rs.at[x], x_peer(dd)) for dd in (2, 1, 3)]
        start_all(q_send)

        def iota(shape, d):
            return lax.broadcasted_iota(jnp.int32, shape, d)

        i0, i1 = iota((256, 256), 0), iota((256, 256), 1)
        pick = jnp.where(i1 == (i0 & 63) * KV + lax.shift_right_logical(i0, 6), 1.0, 0.0).astype(BF)
        for cpy in local[1:]:
            cpy.wait()
        groups = cache // 128
        unroll = max(u for u in (1, 2, 4) if groups % u == 0)

        def split(g0, _):
            for du in range(unroll):
                g = g0 * unroll + du
                for raw, dst, flip in ((kraw, kh, False), (vraw, vh, True)):
                    rows = raw[pl.ds(pl.multiple_of(g * 128 * KV, 256), 128 * KV), :]
                    both = jnp.concatenate([rows[:256], rows[256:]], axis=1)
                    r = jnp.dot(pick, both, preferred_element_type=F32).astype(BF)
                    for h in range(KV):
                        one = jnp.concatenate([r[h * 64:(h + 1) * 64, :128], r[h * 64:(h + 1) * 64, 128:]], axis=0)
                        dst[h, pl.ds(pl.multiple_of(g * 128, 128), 128), :] = one.T if flip else one
            return 0

        lax.fori_loop(0, groups // unroll, split, 0)
        kb[own, :] = kh[x]
        vb[own, :] = vh[x]
        n0, n1 = iota((KV * PAD, tok * KV), 0), iota((KV * PAD, tok * KV), 1)
        npick = jnp.where((n0 % PAD < tok) & (n1 == (n0 % PAD) * KV + n0 // PAD), 1.0, 0.0).astype(BF)
        for i, raw in enumerate((knraw, vnraw)):
            r = jnp.dot(npick, raw[...], preferred_element_type=F32).astype(BF)
            for h in range(KV):
                nh[h, i] = r[h * PAD:(h + 1) * PAD]
        nrecv[me_j] = nh[x]

        def kv_copies(dd):
            slot = ((XD - dd) % XD) * 2 + c
            there = pl.ds(slot * cache, cache)
            dev = x_peer(dd) if dd else mate
            return [rc(src.at[(x + dd) % XD], dst.at[there], k_ss.at[dd, i], k_rs.at[slot, i], dev)
                    for i, (src, dst) in enumerate(((kh, kb), (vh, vb)))]

        kv_send = kv_copies(0)
        kv_send += [rc(kh.at[(x + 2) % XD], rk, r_ss.at[0], r_rs.at[0], x_peer(1)),
                    rc(vh.at[(x + 2) % XD], rv, r_ss.at[1], r_rs.at[1], x_peer(3))]
        kv_send += kv_copies(1) + kv_copies(3)
        n_send = [rc(nh.at[(x + dd) % XD], nrecv.at[me_j], n_ss.at[i], n_rs.at[me_j], row_peer(dd, dc))
                  for i, (dd, dc) in enumerate(row_devs)]
        for cpy in kv_send + n_send:
            cpy.start()
        there = pl.ds((2 * 2 + c) * cache, cache)
        kv_relay = [rc(rk, kb.at[there], h_ss.at[0], k_rs.at[2 * 2 + c, 0], x_peer(1)),
                    rc(rv, vb.at[there], h_ss.at[1], k_rs.at[2 * 2 + c, 1], x_peer(3))]

        for dd in range(1, XD):
            src = (x + dd) % XD
            rc(qv.at[x], qx.at[src], q_ss.at[dd], q_rs.at[src], x_peer(dd)).wait_recv()

        def joined(pieces):
            return jnp.concatenate([v.astype(F32) for v in pieces], axis=0).astype(BF)

        qx[x] = qv[x]
        qall[pl.ds(0, UNIT), :] = joined([qx[i] for i in range(XD)])
        def half(w, h):
            start = w * UNIT + h * HALF
            return pl.ds(start if isinstance(w, int) else pl.multiple_of(start, 16), SIZE[h])

        b_send, late_send = (
            [rc(qall.at[half(0, h)], qall.at[half(w, h)], b_ss.at[2 * w + h], b_rs.at[2 * w + h], from_peer(w))
             for h in range(2) for w in ws] for ws in (straight, late))
        start_all(b_send)
        w_send = []
        for i, (hw, sy, sz, there_w) in enumerate(onward):
            w, h = hw // 2, hw % 2
            dev = at(x, (y + YD + sy) % YD, (z + ZD + sz) % ZD, c)
            w_send.append(rc(qall.at[half(w, h)], qall.at[half(there_w, h)], w_ss.at[i], b_rs.at[2 * there_w + h], dev))

        prefix = plen[0]
        riota = iota((256, 128), 0)
        lane0 = iota((256, 128), 1) == 0
        nblk = cache // 256

        def bias_block(b, _):
            slot = b // nblk
            base = ((row0 + (x + slot // 2) % XD) * 2 + slot % 2) * cache + (b % nblk) * 256
            hide = jnp.where(lane0 & (riota + base >= prefix), FILL, 0.0)
            bias[pl.ds(pl.multiple_of(b * 256, 256), 256), :] = hide.astype(BF)
            return 0

        lax.fori_loop(0, NCB, bias_block, 0)
        bias[pl.ds(NCB * 256, 256), :] = jnp.zeros((256, 128), BF)
        dev_j = lax.shift_right_logical(riota, 5)
        r_j = lax.bitwise_and(riota, PAD - 1)
        keyid[...] = jnp.where(r_j < tok, (row0 * 2 + dev_j) * tok + r_j, 1 << 23).astype(F32)

        r = (iota((NPAIR * 2, 256), 0) * 256 + iota((NPAIR * 2, 256), 1)).astype(F32)

        def parts(v, n):
            d = jnp.floor((v + 0.5) * (1.0 / n))
            return d, v - d * n

        unit_no, rest = parts(r, UNIT)
        chip_no, rest = parts(rest, PIECE)
        _, tok_no = parts(rest, tok)
        chip_row = jnp.zeros_like(r)
        for w, (dy, dz) in enumerate(offs):
            first_chip = ((z + dz) % ZD * YD + (y + dy) % YD) * XD
            chip_row = jnp.where(unit_no == w, first_chip.astype(F32), chip_row)
        tq[...] = ((chip_row + chip_no) * 2.0 + c.astype(F32)) * tok + tok_no

        def arrived(w, h):
            rc(qall.at[half(0, h)], qall.at[half(w, h)], b_ss.at[2 * w + h], b_rs.at[2 * w + h], mate).wait_recv()

        def wait_near(hw):
            arrived(hw // 2, hw % 2)
            for (k, *_), cpy in zip(onward, w_send):
                if k == hw:
                    cpy.start()

        def wait_far(w):
            for h in range(2):
                arrived(w, h)
            relays = {}
            for (k, *_), cpy in zip(onward, w_send):
                if k >= NEAR_END:
                    relays.setdefault(k // 2, []).append(cpy)
            if relays:
                pl.when(w <= max(relays))(lambda: on_value(
                    w, {k: functools.partial(start_all, cpys) for k, cpys in relays.items()}))

        def halves_for(p):
            last = p * 512 + 511
            n = last // UNIT * 2 + 1 + (last % UNIT >= HALF)
            return min(n, 2 * G)

        def units_for(p):
            return jnp.clip((p * 512 + 511) // UNIT + 1, len(straight) + 1, G)

        def prep(p):
            for t in range(2):
                rows = qall[pl.ds(pl.multiple_of((p * 2 + t) * 256, 256), 256), :]
                qt[p * 2 + t] = rows.T

        ones_row = jnp.where(iota((128, 256), 0) == 0, 1.0, 0.0).astype(BF)

        def rep(v, n):
            return jnp.concatenate([v] * n, axis=0)

        def finish(p):
            for t in range(2):
                tile = p * 2 + t
                m = mraw[t]
                alpha = jnp.exp2((mb[tile] - m) * SCALE2)
                l = jnp.sum(lraw[t] + alpha * lb[tile], axis=0, keepdims=True)
                inv = 1.0 / l
                o = (oacc[tile] * rep(alpha, 16) + oraw[t]) * inv
                obuf[pl.ds(pl.multiple_of(tile * 256, 256), 256), :] = o.T.astype(BF)
                ls = m[0:1] * SCALE2 + jnp.log2(l)
                lbuf[tile * 2] = ls[:, 0:128]
                lbuf[tile * 2 + 1] = ls[:, 128:256]

        def chip_blocks(dx):
            return list(range(dx * CHB, (dx + 1) * CHB))

        blocks_a = chip_blocks(0)
        blocks_near = chip_blocks(1) + chip_blocks(3)
        blocks_far = chip_blocks(2) + [NCB]
        blocks_b = blocks_near + blocks_far

        def unit_body(pv=None, pv_blocks=(), pv_at=0, pv_end="keep", qk=None, qk_blocks=(), qk_at=0, qk_from=None,
                      prep_pair=None, done_pair=None):
            if done_pair is not None:
                finish(done_pair)
            mp = [mcur[t] for t in range(2)]
            lacc = [jnp.zeros((8, 256), F32) for _ in range(2)]
            o = [None, None]
            mxs = [jnp.full((8, 256), -jnp.inf, F32) for _ in range(2)]

            def scores(b, t):
                k = jnp.concatenate([kb[pl.ds(b * 256, 256), :], bias[pl.ds(b * 256, 256), :]], axis=1)
                q = jnp.concatenate([qt[qk * 2 + t], ones_row], axis=0)
                return jnp.dot(k, q, preferred_element_type=F32)

            def keep(i, b, t, s):
                if b == NCB:
                    lim = tq[pl.ds(qk * 2 + t, 1), :]
                    kid = jnp.concatenate([keyid[...], keyid[...]], axis=1)
                    s = jnp.where(kid <= lim, s, FILL)
                sb[t, qk_at + i] = s
                mxs[t] = jnp.maximum(mxs[t], s.reshape(32, 8, 256).max(0))

            def weigh(i, b, t):
                p = jnp.exp2((sb[t, pv_at + i] - rep(mp[t], 32)) * SCALE2)
                lacc[t] = lacc[t] + p.reshape(32, 8, 256).sum(0)
                vt = jnp.concatenate([vb[pl.ds(b * 256, 128), :], vb[pl.ds(b * 256 + 128, 128), :]], axis=1)
                d = jnp.dot(vt, p.astype(BF), preferred_element_type=F32)
                o[t] = d if o[t] is None else o[t] + d

            for i in range(max(len(pv_blocks), len(qk_blocks))):
                for t in range(2):
                    if i < len(qk_blocks) and t == 0:
                        s = scores(qk_blocks[i], t)
                    if i < len(pv_blocks):
                        weigh(i, pv_blocks[i], t)
                    if i < len(qk_blocks):
                        keep(i, qk_blocks[i], t, s if t == 0 else scores(qk_blocks[i], t))
            if pv is not None:
                for t in range(2):
                    tile = pv * 2 + t
                    if pv_end == "keep":
                        oacc[tile] = o[t]
                        lb[tile] = lacc[t]
                    elif pv_end == "add":
                        alpha = jnp.exp2((mb[tile] - mp[t]) * SCALE2)
                        oacc[tile] = oacc[tile] * rep(alpha, 16) + o[t]
                        lb[tile] = lb[tile] * alpha + lacc[t]
                        mb[tile] = mp[t]
                    else:
                        oraw[t] = o[t]
                        lraw[t] = lacc[t]
                        mraw[t] = mp[t]
            if prep_pair is not None:
                prep(prep_pair)
            if qk is not None:
                for t in range(2):
                    m = jnp.broadcast_to(jnp.max(mxs[t], axis=0, keepdims=True), (8, 256))
                    if qk_from is None:
                        mb[qk * 2 + t] = m
                    else:
                        m = jnp.maximum(m, mp[t] if qk_from is mcur else mb[qk * 2 + t])
                    mcur[t] = m

        def compute():
            other = pl.ds((1 - c) * cache, cache)
            for i, (src, dst) in enumerate(((kh, kb), (vh, vb))):
                rc(src.at[x], dst.at[other], k_ss.at[0, i], k_rs.at[1 - c, i], mate).wait_recv()
            prep(0)
            unit_body(qk=0, qk_blocks=blocks_a)
            first_end = halves_for(min(1, NPAIR - 1))
            for hw in range(2, first_end):
                wait_near(hw)
            prep(1)

            def forwarded(dx, cc):
                there = pl.ds((dx * 2 + cc) * cache, cache)
                return [rc(buf.at[there], buf.at[there], f_ss.at[dx, i], k_rs.at[dx * 2 + cc, i], mate)
                        for i, buf in enumerate((kb, vb))]

            def forward(dxs):
                for dx in dxs:
                    for cpy in forwarded(dx, c):
                        cpy.wait_recv()
                        cpy.start()

            def pass_a(u, _):
                have, need = units_for(u + 1), units_for(u + 2)
                pl.when(need > have)(lambda: wait_far(have))

                @pl.when(u == min(3, NPAIR - 2))
                def _():
                    for i, buf in enumerate((rk, rv)):
                        rc(buf, buf, r_ss.at[i], r_rs.at[i], mate).wait_recv()
                        kv_relay[i].start()

                @pl.when(u == min(14, NPAIR - 2))
                def _():
                    forward((1, 3))

                unit_body(pv=u, pv_blocks=blocks_a, qk=u + 1, qk_blocks=blocks_a,
                          prep_pair=jnp.minimum(u + 2, NPAIR - 1))
                return 0

            unit_body(pv=0, pv_blocks=blocks_a, qk=1, qk_blocks=blocks_a)
            for hw in range(first_end, NEAR_END):
                wait_near(hw)
            start_all(late_send)
            for w in range(len(straight) + 1, (halves_for(2) + 1) // 2):
                wait_far(jnp.int32(w))
            prep(2)
            lax.fori_loop(1, NPAIR - 1, pass_a, 0)

            def mate_has(dxs):
                for dx in dxs:
                    for cpy in forwarded(dx, 1 - c):
                        cpy.wait_recv()

            last = NPAIR - 1
            mate_has((1, 3))
            forward((2,))
            unit_body(pv=last, pv_blocks=blocks_a, qk=last, qk_blocks=blocks_near, qk_from=mb)
            for i in range(1, 8):
                j = (me_j + i) % 8
                rc(nh.at[x], nrecv.at[j], n_ss.at[0], n_rs.at[j], mate).wait_recv()
            newv = jnp.concatenate([nrecv[j, 1] for j in range(8)], axis=0).T
            kb[pl.ds(NCB * 256, 256), :] = jnp.concatenate([nrecv[j, 0] for j in range(8)], axis=0)
            vb[pl.ds(NCB * 256, 128), :] = newv[:, 0:128]
            vb[pl.ds(NCB * 256 + 128, 128), :] = newv[:, 128:256]
            mate_has((2,))
            unit_body(qk=last, qk_blocks=blocks_far, qk_at=len(blocks_near), qk_from=mcur)

            def copies_done(pairs):
                return [cpy for w in range(1, G) for h in range(2) if (w * UNIT + h * HALF) // 512 in pairs
                        for cpy in out_copies(w, h)]

            leave, prev = {}, NPAIR
            for u in sorted({NPAIR - 3 - d for d in (0, 1, 3, 5, 8, 12, 16) if NPAIR - 3 - d >= 1}):
                leave[u] = functools.partial(start_all, copies_done(range(NPAIR - u, prev)))
                prev = NPAIR - u

            def pass_b(u, _):
                p = last - u
                unit_body(pv=p, pv_blocks=blocks_b, pv_end="last", qk=p - 1, qk_blocks=blocks_b, qk_from=mb,
                          done_pair=jnp.minimum(p + 1, last))
                on_value(u, leave)
                return 0

            lax.fori_loop(0, NPAIR - 2, pass_b, 0)
            cut = (len(blocks_b) + 1) // 2
            unit_body(pv=1, pv_blocks=blocks_b, pv_end="last", qk=0, qk_blocks=blocks_b[:cut], qk_from=mb,
                      done_pair=min(2, last))
            finish(1)
            start_all(copies_done(range(1, prev)))
            unit_body(pv=0, pv_blocks=blocks_b[:cut], pv_end="add", qk=0, qk_blocks=blocks_b[cut:], qk_at=cut, qk_from=mcur)
            unit_body(pv=0, pv_blocks=blocks_b[cut:], pv_at=cut, pv_end="last")
            finish(0)
            start_all(copies_done([0]))

        def out_copies(w, h):
            cpys = [rc(obuf.at[half(w, h)], orecv.at[w, half(0, h)], o_ss.at[2 * w + h], o_rs.at[2 * w + h], to_peer(w))]
            if h == 0:
                e0 = (w * UNIT) // 128
                cpys.append(rc(lbuf.at[pl.ds(e0, LSE_ROWS)], lrecv.at[w], l_ss.at[w], l_rs.at[w], to_peer(w)))
            return cpys

        compute()

        for w in range(1, G):
            for h in range(2):
                for cpy in out_copies(w, h):
                    cpy.wait_recv()
        lane = iota((LSE_ROWS, 128), 1)

        def shifted(v, off):
            if off == 0:
                return v
            r = pltpu.roll(v, 128 - off, 1)
            nxt = jnp.concatenate([r[1:], r[-1:]], axis=0)
            return jnp.where(lane[: v.shape[0]] < 128 - off, r, nxt)

        def lse_of(w):
            v = lbuf[pl.ds(0, LSE_ROWS)] if w == 0 else lrecv[w]
            return shifted(v.reshape(LSE_ROWS, 128), (w * UNIT) % 128)

        lses = [lse_of(w) for w in range(G)]
        top = functools.reduce(jnp.maximum, lses)
        wts = [jnp.exp2(v - top) for v in lses]
        den = functools.reduce(jnp.add, wts)
        inv = 1.0 / den
        wts = [v * inv for v in wts]
        total = (top + jnp.log2(den)) * LN2
        def bf(v):
            return v.astype(BF).astype(F32)

        cols = []
        for j in range(-(-UNIT // 128)):
            rows = jnp.concatenate([v[j:j + 1] for v in wts], axis=0)
            mid = rows - bf(rows)
            stack = [bf(rows), bf(mid), bf(mid - bf(mid)), jnp.zeros((128 - 3 * G, 128), F32)]
            cols.append(jnp.concatenate(stack, axis=0).T.astype(BF))
        cols = jnp.concatenate(cols, axis=0)[:UNIT]
        k0, k1 = iota((128, 256), 0), iota((128, 256), 1)
        final = jnp.zeros((UNIT, 128), F32)
        for w0 in range(0, G, 2):
            spread = jnp.where((k0 < 3 * G) & (k0 % G == w0 + lax.shift_right_logical(k1, 7)), 1.0, 0.0).astype(BF)
            lanes = jnp.dot(cols, spread, preferred_element_type=F32)
            for w in range(w0, min(w0 + 2, G)):
                src = obuf[pl.ds(0, UNIT), :] if w == 0 else orecv[w]
                final = final + src.astype(F32) * lanes[:, (w - w0) * 128:(w - w0 + 1) * 128]
        for i in range(XD):
            fo[i] = final[i * PIECE:(i + 1) * PIECE].astype(BF)
            off = (i * PIECE) % 128
            e = (i * PIECE) // 128
            need = min(3, LSE_ROWS - e)
            v = shifted(total[e:e + need], off)
            v = v if need >= 2 else jnp.concatenate([v, v], axis=0)
            fl[2 * i] = v[0:1]
            fl[2 * i + 1] = v[1:2]
        x_send = []
        for dd in range(1, XD):
            xd = (x + dd) % XD
            x_send.append(rc(fo.at[xd], out.at[x], x_ss.at[dd], x_rs.at[x], x_peer(dd)))
            x_send.append(rc(fl.at[pl.ds(2 * xd, 2)], lse_out.at[pl.ds(2 * x, 2)], y_ss.at[dd], y_rs.at[x], x_peer(dd)))
        for cpy in x_send:
            cpy.start()
        mine = pltpu.make_async_copy(fo.at[x], out.at[x], lsem.at[0])
        mine.start()
        lse_copy = pltpu.make_async_copy(fl.at[pl.ds(2 * x, 2)], lse_out.at[pl.ds(2 * x, 2)], lsem.at[1])
        lse_copy.start()
        for dd in range(1, XD):
            src = (x + dd) % XD
            rc(fl.at[pl.ds(0, 2)], lse_out.at[pl.ds(2 * src, 2)], y_ss.at[dd], y_rs.at[src], x_peer(dd)).wait_recv()
        for cpy in q_send + kv_send + kv_relay + n_send + b_send + late_send + w_send + x_send:
            cpy.wait_send()
        for dx in range(1, XD):
            m = pl.ds((dx * 2 + c) * cache, cache)
            for i, buf in enumerate((kb, vb)):
                rc(buf.at[m], buf.at[m], f_ss.at[dx, i], k_rs.at[dx * 2 + c, i], mate).wait_send()
        for w in range(1, G):
            for cpy in out_copies(w, 0) + out_copies(w, 1):
                cpy.wait_send()
        for dd in range(1, XD):
            src = (x + dd) % XD
            rc(fo.at[0], out.at[src], x_ss.at[dd], x_rs.at[src], x_peer(dd)).wait_recv()
        mine.wait()
        lse_copy.wait()

    D, R = pltpu.SemaphoreType.DMA, NPAIR * 2
    V = pltpu.VMEM
    scratch = [
        V((XD, PIECE, 128), BF), V((cache * KV, 128), BF), V((cache * KV, 128), BF),
        V((tok * KV, 128), BF), V((tok * KV, 128), BF),
        V((KV, cache, 128), BF), V((KV, cache, 128), BF), V((KV, 2, PAD, 128), BF),
        V((cache, 128), BF), V((cache, 128), BF),
        V((NKB * 256, 128), BF), V((NKB * 256, 128), BF), V((NKB * 256, 128), BF),
        V((XD, PIECE, 128), BF),
        V((NPAIR * 512, 128), BF), V((R, 128, 256), BF),
        V((2, NKB - CHB, 256, 256), F32), V((R, 128, 256), F32),
        V((R, 8, 256), F32), V((R, 8, 256), F32), V((2, 8, 256), F32),
        V((2, 128, 256), F32), V((2, 8, 256), F32), V((2, 8, 256), F32), V((R, 256), F32),
        V((256, 128), F32), V((8, 2, PAD, 128), BF),
        V((NPAIR * 512, 128), BF), V((R * 2 + LSE_ROWS, 1, 128), F32),
        V((G, UNIT, 128), BF), V((G, LSE_ROWS, 1, 128), F32),
        V((XD, PIECE, 128), BF), V((2 * XD, 1, 128), F32),
        D((5,)), D((XD,)), D((XD,)), D((2 * G,)), D((2 * G,)), D((max(1, len(onward)),)),
        D((XD, 2)), D((2 * XD, 2)), D((XD, 2)), D((2,)), D((2,)), D((2,)), D((7,)), D((8,)),
        D((2 * G,)), D((2 * G,)), D((G,)), D((G,)), D((XD,)), D((XD,)), D((XD,)), D((XD,)),
    ]
    any_ = pl.BlockSpec(memory_space=pl.ANY)
    return pl.pallas_call(
        kernel,
        out_shape=(jax.ShapeDtypeStruct((XD, PIECE, 128), BF), jax.ShapeDtypeStruct((2 * XD, 1, 128), F32)),
        in_specs=[pl.BlockSpec(memory_space=pltpu.SMEM)] + [any_] * 5,
        out_specs=(any_, any_),
        scratch_shapes=scratch,
        name="prefix_attention",
        compiler_params=pltpu.CompilerParams(collective_id=0, has_side_effects=True, vmem_limit_bytes=63 << 20),
    )


def make_finish(tok):
    rows = RATIO * tok

    def kernel(o_in, l_in, o_out, l_out, o_buf, l_buf, table, sem):
        o_get = pltpu.make_async_copy(o_in, o_buf, sem.at[0])
        l_get = pltpu.make_async_copy(l_in, l_buf, sem.at[1])
        o_get.start()
        l_get.start()
        l_get.wait()
        lane = lax.broadcasted_iota(jnp.int32, (1, 128), 1)
        head_rows = []
        for i in range(KV):
            pair = l_buf[pl.ds(2 * i, 2)].reshape(2, 128)
            for g in range(RATIO):
                s = g * tok
                lo, back = pair[s // 128:s // 128 + 1], 128 - s % 128
                head_rows.append(lo if back == 128 else jnp.where(
                    lane < back, pltpu.roll(lo, back, 1), pltpu.roll(pair[1:2], back, 1)))
        table[...] = jnp.concatenate(head_rows + [jnp.zeros((32 - HEADS, 128), F32)], axis=0).T[:tok, :HEADS]
        l_put = pltpu.make_async_copy(table, l_out, sem.at[2])
        l_put.start()
        o_get.wait()
        o_put = pltpu.make_async_copy(o_buf, o_out, sem.at[3])
        o_put.start()
        l_put.wait()
        o_put.wait()

    V, any_ = pltpu.VMEM, pl.BlockSpec(memory_space=pl.ANY)
    return pl.pallas_call(
        kernel,
        out_shape=(jax.ShapeDtypeStruct((KV, rows, HD), BF), jax.ShapeDtypeStruct((tok, HEADS), F32)),
        in_specs=[any_, any_],
        out_specs=(any_, any_),
        scratch_shapes=[V((KV, rows, HD), BF), V((2 * KV, 1, 128), F32), V((tok, HEADS), F32),
                        pltpu.SemaphoreType.DMA((4,))],
        name="final_form",
    )


def solution(mesh):
    spec = P(("dp", "cp"))

    def local(queries, key_new, value_new, key_cache, value_cache, prefix_len):
        tok, cache = queries.shape[0], key_cache.shape[0]
        call = make_kernel(tok, cache)
        q = queries.transpose(1, 0, 2).reshape(KV, RATIO * tok, HD)

        def rows(a):
            return a.reshape(a.shape[0] * KV, HD)

        out, row_lse = make_finish(tok)(*call(prefix_len, q, rows(key_cache), rows(value_cache), rows(key_new), rows(value_new)))
        return out.reshape(HEADS, tok, HD).transpose(1, 0, 2), row_lse

    return jax.shard_map(local, mesh=mesh, in_specs=(spec,) * 5 + (P("dp"),), out_specs=(spec, spec), check_vma=False)
```

```python
import functools
import math

import jax
import jax.numpy as jnp
from jax import lax
from jax.experimental import pallas as pl
from jax.experimental.pallas import tpu as pltpu
from jax.sharding import PartitionSpec as P

ZD, YD, XD = 4, 4, 4

HEADS, KV, HD = 28, 4, 128
RATIO = HEADS // KV
FILL = -1e30
SCALE2 = HD ** -0.5 * math.log2(math.e)
LN2 = math.log(2.0)
PAD = 32
BF, F32 = jnp.bfloat16, jnp.float32


def ring_offsets():
    def hops(d, n):
        return min(d, n - d)

    offs = [(dy, dz) for dz in range(ZD) for dy in range(YD)]
    return sorted(offs, key=lambda o: (hops(o[0], YD) + hops(o[1], ZD), 0 in o, o[1], o[0]))


def on_value(v, actions):
    keys = sorted(actions)
    if len(keys) == 1:
        pl.when(v == keys[0])(actions[keys[0]])
    elif keys:
        mid = keys[len(keys) // 2]
        pl.when(v < mid)(lambda: on_value(v, {k: a for k, a in actions.items() if k < mid}))
        pl.when(v >= mid)(lambda: on_value(v, {k: a for k, a in actions.items() if k >= mid}))


def make_kernel(tok, cache):
    offs = ring_offsets()
    G = len(offs)
    PIECE = RATIO * tok
    UNIT = XD * PIECE
    ROWS = G * UNIT
    NPAIR = -(-ROWS // 512)
    CHB = 2 * cache // 256
    NCB = XD * CHB
    NKB = NCB + 1
    HALF = (UNIT // 2 + 31) // 32 * 32 if UNIT > 512 else UNIT // 2
    SIZE = (HALF, UNIT - HALF)
    assert HALF % 16 == 0 and UNIT % 16 == 0
    slot_of = {o: w for w, o in enumerate(offs)}
    straight = [w for w, o in enumerate(offs) if w and 0 in o and 2 not in o]
    late = [w for w, o in enumerate(offs) if o == (2, 2)]
    assert straight == list(range(1, len(straight) + 1))

    def toward(d, n):
        return 1 if d <= n // 2 else -1

    onward = []
    for w, (ty, tz) in enumerate(offs):
        if w == 0 or w in straight or w in late:
            continue
        if YD == 4 and ty == 2:
            via = [(1, 0), (-1, 0)]
        elif ZD == 4 and tz == 2:
            via = [(0, 1), (0, -1)]
        else:
            via = [(toward(ty, YD), 0), (0, toward(tz, ZD))]
        for h, (ny, nz) in enumerate(via):
            onward.append((2 * slot_of[(ty - ny) % YD, (tz - nz) % ZD] + h, -ny, -nz, w))
    onward.sort()
    NEAR_END = 2 * (len(straight) + 1)
    LSE_ROWS = UNIT // 128 + 1
    assert cache % 256 == 0 and 8 * PAD == 256 and tok <= PAD

    def kernel(plen, q_in, k_in, v_in, kn_in, vn_in, out, lse_out,
               qv, kraw, vraw, knraw, vnraw, kh, vh, nh, rk, rv,
               kb, vb, bias, qx, qall, qt, sb, oacc, mb, lb, mcur, oraw, lraw, mraw, tq, keyid, nrecv,
               obuf, lbuf, orecv, lrecv, fo, fl,
               lsem, q_ss, q_rs, b_ss, b_rs, w_ss, k_ss, k_rs, f_ss, r_ss, r_rs, h_ss, n_ss, n_rs,
               o_ss, o_rs, l_ss, l_rs, x_ss, x_rs, y_ss, y_rs):
        cp = lax.axis_index("cp")
        c = cp % 2
        x = (cp // 2) % XD
        y = (cp // (2 * XD)) % YD
        z = cp // (2 * XD * YD)
        row0 = (z * YD + y) * XD

        def at(xx, yy, zz, cc):
            return ((zz * YD + yy) * XD + xx) * 2 + cc

        def x_peer(dd):
            return at((x + dd) % XD, y, z, c)

        mate = at(x, y, z, 1 - c)

        def to_peer(w):
            dy, dz = offs[w]
            return at(x, (y + dy) % YD, (z + dz) % ZD, c)

        def from_peer(w):
            dy, dz = offs[w]
            return at(x, (y + YD - dy) % YD, (z + ZD - dz) % ZD, c)

        def start_all(cpys):
            for cpy in cpys:
                cpy.start()

        def rc(src, dst, ss, rs, dev):
            return pltpu.make_async_remote_copy(
                src_ref=src, dst_ref=dst, send_sem=ss, recv_sem=rs,
                device_id={"cp": dev}, device_id_type=pl.DeviceIdType.MESH)

        row_devs = [(dd, dc) for dd in range(XD) for dc in range(2) if (dd, dc) != (0, 0)]

        def row_peer(dd, dc):
            return at((x + dd) % XD, y, z, (c + dc) % 2)

        barrier = pltpu.get_barrier_semaphore()
        peers = [to_peer(w) for w in range(1, G)] + [row_peer(dd, dc) for dd, dc in row_devs]
        for p in peers:
            pl.semaphore_signal(barrier, inc=1, device_id={"cp": p}, device_id_type=pl.DeviceIdType.MESH)
        me_j = x * 2 + c
        own = pl.ds(c * cache, cache)
        local = [pltpu.make_async_copy(src, dst, lsem.at[i]) for i, (src, dst) in enumerate(
            [(q_in, qv), (k_in, kraw), (v_in, vraw), (kn_in, knraw), (vn_in, vnraw)])]
        for cpy in local:
            cpy.start()
        local[0].wait()
        pl.semaphore_wait(barrier, len(peers))

        q_send = [rc(qv.at[(x + dd) % XD], qx.at[x], q_ss.at[dd], q_rs.at[x], x_peer(dd)) for dd in (2, 1, 3)]
        start_all(q_send)

        def iota(shape, d):
            return lax.broadcasted_iota(jnp.int32, shape, d)

        i0, i1 = iota((256, 256), 0), iota((256, 256), 1)
        pick = jnp.where(i1 == (i0 & 63) * KV + lax.shift_right_logical(i0, 6), 1.0, 0.0).astype(BF)
        for cpy in local[1:]:
            cpy.wait()
        groups = cache // 128
        unroll = max(u for u in (1, 2, 4) if groups % u == 0)

        def split(g0, _):
            for du in range(unroll):
                g = g0 * unroll + du
                for raw, dst, flip in ((kraw, kh, False), (vraw, vh, True)):
                    rows = raw[pl.ds(pl.multiple_of(g * 128 * KV, 256), 128 * KV), :]
                    both = jnp.concatenate([rows[:256], rows[256:]], axis=1)
                    r = jnp.dot(pick, both, preferred_element_type=F32).astype(BF)
                    for h in range(KV):
                        one = jnp.concatenate([r[h * 64:(h + 1) * 64, :128], r[h * 64:(h + 1) * 64, 128:]], axis=0)
                        dst[h, pl.ds(pl.multiple_of(g * 128, 128), 128), :] = one.T if flip else one
            return 0

        lax.fori_loop(0, groups // unroll, split, 0)
        kb[own, :] = kh[x]
        vb[own, :] = vh[x]
        n0, n1 = iota((KV * PAD, tok * KV), 0), iota((KV * PAD, tok * KV), 1)
        npick = jnp.where((n0 % PAD < tok) & (n1 == (n0 % PAD) * KV + n0 // PAD), 1.0, 0.0).astype(BF)
        for i, raw in enumerate((knraw, vnraw)):
            r = jnp.dot(npick, raw[...], preferred_element_type=F32).astype(BF)
            for h in range(KV):
                nh[h, i] = r[h * PAD:(h + 1) * PAD]
        nrecv[me_j] = nh[x]

        def kv_copies(dd):
            slot = ((XD - dd) % XD) * 2 + c
            there = pl.ds(slot * cache, cache)
            dev = x_peer(dd) if dd else mate
            return [rc(src.at[(x + dd) % XD], dst.at[there], k_ss.at[dd, i], k_rs.at[slot, i], dev)
                    for i, (src, dst) in enumerate(((kh, kb), (vh, vb)))]

        kv_send = kv_copies(0)
        kv_send += [rc(kh.at[(x + 2) % XD], rk, r_ss.at[0], r_rs.at[0], x_peer(1)),
                    rc(vh.at[(x + 2) % XD], rv, r_ss.at[1], r_rs.at[1], x_peer(3))]
        kv_send += kv_copies(1) + kv_copies(3)
        n_send = [rc(nh.at[(x + dd) % XD], nrecv.at[me_j], n_ss.at[i], n_rs.at[me_j], row_peer(dd, dc))
                  for i, (dd, dc) in enumerate(row_devs)]
        for cpy in kv_send + n_send:
            cpy.start()
        there = pl.ds((2 * 2 + c) * cache, cache)
        kv_relay = [rc(rk, kb.at[there], h_ss.at[0], k_rs.at[2 * 2 + c, 0], x_peer(1)),
                    rc(rv, vb.at[there], h_ss.at[1], k_rs.at[2 * 2 + c, 1], x_peer(3))]

        for dd in range(1, XD):
            src = (x + dd) % XD
            rc(qv.at[x], qx.at[src], q_ss.at[dd], q_rs.at[src], x_peer(dd)).wait_recv()

        def joined(pieces):
            return jnp.concatenate([v.astype(F32) for v in pieces], axis=0).astype(BF)

        qx[x] = qv[x]
        qall[pl.ds(0, UNIT), :] = joined([qx[i] for i in range(XD)])
        def half(w, h):
            start = w * UNIT + h * HALF
            return pl.ds(start if isinstance(w, int) else pl.multiple_of(start, 16), SIZE[h])

        b_send, late_send = (
            [rc(qall.at[half(0, h)], qall.at[half(w, h)], b_ss.at[0], b_rs.at[2 * w + h], from_peer(w))
             for h in range(2) for w in ws] for ws in (straight, late))
        start_all(b_send)
        w_send = []
        for i, (hw, sy, sz, there_w) in enumerate(onward):
            w, h = hw // 2, hw % 2
            dev = at(x, (y + YD + sy) % YD, (z + ZD + sz) % ZD, c)
            w_send.append(rc(qall.at[half(w, h)], qall.at[half(there_w, h)], w_ss.at[0], b_rs.at[2 * there_w + h], dev))

        prefix = plen[0]
        riota = iota((256, 128), 0)
        per = cache // 256
        fill = jnp.where(iota((8, 128), 1) == 0, FILL, 0.0)

        def bias_slot(slot, _):
            base = ((row0 + (x + slot // 2) % XD) * 2 + slot % 2) * cache
            for b in range(per):
                hide = [jnp.where(riota[r * 8:r * 8 + 8] >= prefix - base - b * 256, fill, 0.0) for r in range(32)]
                at_b = pl.multiple_of((slot * per + b) * 256, 256)
                bias[pl.ds(at_b, 256), :] = jnp.concatenate(hide, axis=0).astype(BF)
            return 0

        lax.fori_loop(0, 2 * XD, bias_slot, 0)
        bias[pl.ds(NCB * 256, 256), :] = jnp.zeros((256, 128), BF)
        dev_j = lax.shift_right_logical(riota, 5)
        r_j = lax.bitwise_and(riota, PAD - 1)
        keyid[...] = jnp.where(r_j < tok, (row0 * 2 + dev_j) * tok + r_j, 1 << 23).astype(F32)

        r = (iota((NPAIR * 2, 256), 0) * 256 + iota((NPAIR * 2, 256), 1)).astype(F32)

        def parts(v, n):
            d = jnp.floor((v + 0.5) * (1.0 / n))
            return d, v - d * n

        unit_no, rest = parts(r, UNIT)
        chip_no, rest = parts(rest, PIECE)
        _, tok_no = parts(rest, tok)
        chip_row = jnp.zeros_like(r)
        for w, (dy, dz) in enumerate(offs):
            first_chip = ((z + dz) % ZD * YD + (y + dy) % YD) * XD
            chip_row = jnp.where(unit_no == w, first_chip.astype(F32), chip_row)
        tq[...] = ((chip_row + chip_no) * 2.0 + c.astype(F32)) * tok + tok_no

        def arrived(w, h):
            rc(qall.at[half(0, h)], qall.at[half(w, h)], b_ss.at[0], b_rs.at[2 * w + h], mate).wait_recv()

        def wait_near(hw):
            arrived(hw // 2, hw % 2)
            for (k, *_), cpy in zip(onward, w_send):
                if k == hw:
                    cpy.start()

        def wait_far(w):
            for h in range(2):
                arrived(w, h)
            relays = {}
            for (k, *_), cpy in zip(onward, w_send):
                if k >= NEAR_END:
                    relays.setdefault(k // 2, []).append(cpy)
            if relays:
                pl.when(w <= max(relays))(lambda: on_value(
                    w, {k: functools.partial(start_all, cpys) for k, cpys in relays.items()}))

        def halves_for(p):
            last = p * 512 + 511
            n = last // UNIT * 2 + 1 + (last % UNIT >= HALF)
            return min(n, 2 * G)

        def units_for(p):
            return jnp.clip((p * 512 + 511) // UNIT + 1, len(straight) + 1, G)

        def prep(p):
            for t in range(2):
                rows = qall[pl.ds(pl.multiple_of((p * 2 + t) * 256, 256), 256), :]
                qt[p * 2 + t] = rows.T

        ones_row = jnp.where(iota((128, 256), 0) == 0, 1.0, 0.0).astype(BF)

        def rep(v, n):
            return jnp.concatenate([v] * n, axis=0)

        def finish(p):
            for t in range(2):
                tile = p * 2 + t
                m = mraw[t]
                alpha = jnp.exp2((mb[tile] - m) * SCALE2)
                l = jnp.sum(lraw[t] + alpha * lb[tile], axis=0, keepdims=True)
                inv = 1.0 / l
                o = (oacc[tile] * rep(alpha, 16) + oraw[t]) * inv
                obuf[pl.ds(pl.multiple_of(tile * 256, 256), 256), :] = o.T.astype(BF)
                ls = m[0:1] * SCALE2 + jnp.log2(l)
                lbuf[tile * 2] = ls[:, 0:128]
                lbuf[tile * 2 + 1] = ls[:, 128:256]

        def chip_blocks(dx):
            return list(range(dx * CHB, (dx + 1) * CHB))

        blocks_a = chip_blocks(0)
        blocks_near = chip_blocks(1) + chip_blocks(3)
        blocks_far = chip_blocks(2) + [NCB]
        blocks_b = blocks_near + blocks_far

        def unit_body(pv=None, pv_blocks=(), pv_end="keep", qk=None, qk_blocks=(), qk_at=0, qk_from=None,
                      prep_pair=None, done_pair=None):
            if done_pair is not None:
                finish(done_pair)
            mp = [mcur[t] for t in range(2)]
            lacc = [jnp.zeros((8, 256), F32) for _ in range(2)]
            o = [None, None]
            mxs = [jnp.full((8, 256), -jnp.inf, F32) for _ in range(2)]

            def scores(b, t):
                k = jnp.concatenate([kb[pl.ds(b * 256, 256), :], bias[pl.ds(b * 256, 256), :]], axis=1)
                q = jnp.concatenate([qt[qk * 2 + t], ones_row], axis=0)
                return jnp.dot(k, q, preferred_element_type=F32)

            def keep(i, b, t, s):
                if b == NCB:
                    lim = tq[pl.ds(qk * 2 + t, 1), :]
                    kid = jnp.concatenate([keyid[...], keyid[...]], axis=1)
                    s = jnp.where(kid <= lim, s, FILL)
                sb[t, qk_at + i] = s
                mxs[t] = jnp.maximum(mxs[t], s.reshape(32, 8, 256).max(0))

            def weigh(i, b, t):
                p = jnp.exp2((sb[t, i] - rep(mp[t], 32)) * SCALE2)
                lacc[t] = lacc[t] + p.reshape(32, 8, 256).sum(0)
                vt = jnp.concatenate([vb[pl.ds(b * 256, 128), :], vb[pl.ds(b * 256 + 128, 128), :]], axis=1)
                d = jnp.dot(vt, p.astype(BF), preferred_element_type=F32)
                o[t] = d if o[t] is None else o[t] + d

            for i in range(max(len(pv_blocks), len(qk_blocks))):
                for t in range(2):
                    if i < len(qk_blocks) and t == 0:
                        s = scores(qk_blocks[i], t)
                    if i < len(pv_blocks):
                        weigh(i, pv_blocks[i], t)
                    if i < len(qk_blocks):
                        keep(i, qk_blocks[i], t, s if t == 0 else scores(qk_blocks[i], t))
            if pv is not None:
                for t in range(2):
                    tile = pv * 2 + t
                    if pv_end == "keep":
                        oacc[tile] = o[t]
                        lb[tile] = lacc[t]
                    else:
                        oraw[t] = o[t]
                        lraw[t] = lacc[t]
                        mraw[t] = mp[t]
            if prep_pair is not None:
                prep(prep_pair)
            if qk is not None:
                for t in range(2):
                    m = jnp.broadcast_to(jnp.max(mxs[t], axis=0, keepdims=True), (8, 256))
                    if qk_from is None:
                        mb[qk * 2 + t] = m
                    else:
                        m = jnp.maximum(m, mp[t] if qk_from is mcur else mb[qk * 2 + t])
                    mcur[t] = m

        def compute():
            other = pl.ds((1 - c) * cache, cache)
            for i, (src, dst) in enumerate(((kh, kb), (vh, vb))):
                rc(src.at[x], dst.at[other], k_ss.at[0, i], k_rs.at[1 - c, i], mate).wait_recv()
            prep(0)
            unit_body(qk=0, qk_blocks=blocks_a)
            first_end = halves_for(min(1, NPAIR - 1))
            for hw in range(2, first_end):
                wait_near(hw)
            prep(1)

            def forwarded(dx, cc):
                there = pl.ds((dx * 2 + cc) * cache, cache)
                return [rc(buf.at[there], buf.at[there], f_ss.at[dx, i], k_rs.at[dx * 2 + cc, i], mate)
                        for i, buf in enumerate((kb, vb))]

            def forward(dxs):
                for dx in dxs:
                    for cpy in forwarded(dx, c):
                        cpy.wait_recv()
                        cpy.start()

            def pass_a(u, _):
                have, need = units_for(u + 1), units_for(u + 2)
                pl.when(need > have)(lambda: wait_far(have))

                @pl.when(u == min(3, NPAIR - 2))
                def _():
                    for i, buf in enumerate((rk, rv)):
                        rc(buf, buf, r_ss.at[i], r_rs.at[i], mate).wait_recv()
                        kv_relay[i].start()

                @pl.when(u == min(14, NPAIR - 2))
                def _():
                    forward((1, 3))

                unit_body(pv=u, pv_blocks=blocks_a, qk=u + 1, qk_blocks=blocks_a,
                          prep_pair=jnp.minimum(u + 2, NPAIR - 1))
                return 0

            unit_body(pv=0, pv_blocks=blocks_a, qk=1, qk_blocks=blocks_a)
            for hw in range(first_end, NEAR_END):
                wait_near(hw)
            start_all(late_send)
            for w in range(len(straight) + 1, (halves_for(2) + 1) // 2):
                wait_far(jnp.int32(w))
            prep(2)
            lax.fori_loop(1, NPAIR - 1, pass_a, 0)

            def mate_has(dxs):
                for dx in dxs:
                    for cpy in forwarded(dx, 1 - c):
                        cpy.wait_recv()

            last = NPAIR - 1
            mate_has((1, 3))
            forward((2,))
            unit_body(pv=last, pv_blocks=blocks_a, qk=last, qk_blocks=blocks_near, qk_from=mb)
            for i in range(1, 8):
                j = (me_j + i) % 8
                rc(nh.at[x], nrecv.at[j], n_ss.at[0], n_rs.at[j], mate).wait_recv()
            newv = jnp.concatenate([nrecv[j, 1] for j in range(8)], axis=0).T
            kb[pl.ds(NCB * 256, 256), :] = jnp.concatenate([nrecv[j, 0] for j in range(8)], axis=0)
            vb[pl.ds(NCB * 256, 128), :] = newv[:, 0:128]
            vb[pl.ds(NCB * 256 + 128, 128), :] = newv[:, 128:256]
            mate_has((2,))
            unit_body(qk=last, qk_blocks=blocks_far, qk_at=len(blocks_near), qk_from=mcur)

            def copies_done(pairs):
                return [cpy for w in range(1, G) for h in range(2) if (w * UNIT + h * HALF) // 512 in pairs
                        for cpy in out_copies(w, h)]

            leave, prev = {}, NPAIR
            for u in sorted({NPAIR - 2 - d for d in (0, 1, 2, 4, 6, 9, 13, 17) if NPAIR - 2 - d >= 1}):
                leave[u] = functools.partial(start_all, copies_done(range(NPAIR - u, prev)))
                prev = NPAIR - u

            def pass_b(u, _):
                p = last - u
                unit_body(pv=p, pv_blocks=blocks_b, pv_end="last", qk=p - 1, qk_blocks=blocks_b, qk_from=mb,
                          done_pair=jnp.minimum(p + 1, last))
                on_value(u, leave)
                return 0

            lax.fori_loop(0, NPAIR - 1, pass_b, 0)
            finish(1)
            start_all(copies_done(range(1, prev)))
            unit_body(pv=0, pv_blocks=blocks_b, pv_end="last")
            finish(0)
            start_all(copies_done([0]))

        def out_copies(w, h):
            cpys = [rc(obuf.at[half(w, h)], orecv.at[w, half(0, h)], o_ss.at[0], o_rs.at[0], to_peer(w))]
            if h == 0:
                e0 = (w * UNIT) // 128
                cpys.append(rc(lbuf.at[pl.ds(e0, LSE_ROWS)], lrecv.at[w], l_ss.at[0], l_rs.at[0], to_peer(w)))
            return cpys

        compute()

        def all_out():
            if G == 1:
                return []
            rest = pl.ds(1, G - 1)
            return [rc(orecv.at[rest], orecv.at[rest], o_ss.at[0], o_rs.at[0], mate),
                    rc(lrecv.at[rest], lrecv.at[rest], l_ss.at[0], l_rs.at[0], mate)]

        def all_queries():
            b_rows, w_rows = len(straight + late) * UNIT, sum(SIZE[hw % 2] for hw, *_ in onward)
            return [rc(qall.at[pl.ds(0, n)], qall.at[pl.ds(0, n)], ss.at[0], b_rs.at[0], mate)
                    for n, ss in ((b_rows, b_ss), (w_rows, w_ss)) if n]

        for cpy in all_out():
            cpy.wait_recv()
        lane = iota((LSE_ROWS, 128), 1)

        def shifted(v, off):
            if off == 0:
                return v
            r = pltpu.roll(v, 128 - off, 1)
            nxt = jnp.concatenate([r[1:], r[-1:]], axis=0)
            return jnp.where(lane[: v.shape[0]] < 128 - off, r, nxt)

        def lse_of(w):
            v = lbuf[pl.ds(0, LSE_ROWS)] if w == 0 else lrecv[w]
            return shifted(v.reshape(LSE_ROWS, 128), (w * UNIT) % 128)

        lses = [lse_of(w) for w in range(G)]
        top = functools.reduce(jnp.maximum, lses)
        wts = [jnp.exp2(v - top) for v in lses]
        den = functools.reduce(jnp.add, wts)
        inv = 1.0 / den
        wts = [v * inv for v in wts]
        total = (top + jnp.log2(den)) * LN2
        def bf(v):
            return v.astype(BF).astype(F32)

        cols = []
        for j in range(-(-UNIT // 128)):
            rows = jnp.concatenate([v[j:j + 1] for v in wts], axis=0)
            mid = rows - bf(rows)
            stack = [bf(rows), bf(mid), bf(mid - bf(mid)), jnp.zeros((128 - 3 * G, 128), F32)]
            cols.append(jnp.concatenate(stack, axis=0).T.astype(BF))
        cols = jnp.concatenate(cols, axis=0)[:UNIT]
        k0, k1 = iota((128, 256), 0), iota((128, 256), 1)
        final = jnp.zeros((UNIT, 128), F32)
        for w0 in range(0, G, 2):
            spread = jnp.where((k0 < 3 * G) & (k0 % G == w0 + lax.shift_right_logical(k1, 7)), 1.0, 0.0).astype(BF)
            lanes = jnp.dot(cols, spread, preferred_element_type=F32)
            for w in range(w0, min(w0 + 2, G)):
                src = obuf[pl.ds(0, UNIT), :] if w == 0 else orecv[w]
                final = final + src.astype(F32) * lanes[:, (w - w0) * 128:(w - w0 + 1) * 128]
        for i in range(XD):
            fo[i] = final[i * PIECE:(i + 1) * PIECE].astype(BF)
            off = (i * PIECE) % 128
            e = (i * PIECE) // 128
            need = min(3, LSE_ROWS - e)
            v = shifted(total[e:e + need], off)
            v = v if need >= 2 else jnp.concatenate([v, v], axis=0)
            fl[2 * i] = v[0:1]
            fl[2 * i + 1] = v[1:2]
        x_send = []
        for dd in range(1, XD):
            xd = (x + dd) % XD
            x_send.append(rc(fo.at[xd], out.at[x], x_ss.at[dd], x_rs.at[x], x_peer(dd)))
            x_send.append(rc(fl.at[pl.ds(2 * xd, 2)], lse_out.at[pl.ds(2 * x, 2)], y_ss.at[dd], y_rs.at[x], x_peer(dd)))
        for cpy in x_send:
            cpy.start()
        mine = pltpu.make_async_copy(fo.at[x], out.at[x], lsem.at[0])
        mine.start()
        lse_copy = pltpu.make_async_copy(fl.at[pl.ds(2 * x, 2)], lse_out.at[pl.ds(2 * x, 2)], lsem.at[1])
        lse_copy.start()
        for dd in range(1, XD):
            src = (x + dd) % XD
            rc(fl.at[pl.ds(0, 2)], lse_out.at[pl.ds(2 * src, 2)], y_ss.at[dd], y_rs.at[src], x_peer(dd)).wait_recv()
        for cpy in q_send + kv_send + kv_relay + n_send + x_send + all_queries() + all_out():
            cpy.wait_send()
        for dx in range(1, XD):
            m = pl.ds((dx * 2 + c) * cache, cache)
            for i, buf in enumerate((kb, vb)):
                rc(buf.at[m], buf.at[m], f_ss.at[dx, i], k_rs.at[dx * 2 + c, i], mate).wait_send()
        for dd in range(1, XD):
            src = (x + dd) % XD
            rc(fo.at[0], out.at[src], x_ss.at[dd], x_rs.at[src], x_peer(dd)).wait_recv()
        mine.wait()
        lse_copy.wait()

    D, R = pltpu.SemaphoreType.DMA, NPAIR * 2
    V = pltpu.VMEM
    scratch = [
        V((XD, PIECE, 128), BF), V((cache * KV, 128), BF), V((cache * KV, 128), BF),
        V((tok * KV, 128), BF), V((tok * KV, 128), BF),
        V((KV, cache, 128), BF), V((KV, cache, 128), BF), V((KV, 2, PAD, 128), BF),
        V((cache, 128), BF), V((cache, 128), BF),
        V((NKB * 256, 128), BF), V((NKB * 256, 128), BF), V((NKB * 256, 128), BF),
        V((XD, PIECE, 128), BF),
        V((NPAIR * 512, 128), BF), V((R, 128, 256), BF),
        V((2, NKB - CHB, 256, 256), F32), V((R, 128, 256), F32),
        V((R, 8, 256), F32), V((R, 8, 256), F32), V((2, 8, 256), F32),
        V((2, 128, 256), F32), V((2, 8, 256), F32), V((2, 8, 256), F32), V((R, 256), F32),
        V((256, 128), F32), V((8, 2, PAD, 128), BF),
        V((NPAIR * 512, 128), BF), V((R * 2 + LSE_ROWS, 1, 128), F32),
        V((G, UNIT, 128), BF), V((G, LSE_ROWS, 1, 128), F32),
        V((XD, PIECE, 128), BF), V((2 * XD, 1, 128), F32),
        D((5,)), D((XD,)), D((XD,)), D((1,)), D((2 * G,)), D((1,)),
        D((XD, 2)), D((2 * XD, 2)), D((XD, 2)), D((2,)), D((2,)), D((2,)), D((7,)), D((8,)),
        D((1,)), D((1,)), D((1,)), D((1,)), D((XD,)), D((XD,)), D((XD,)), D((XD,)),
    ]
    any_ = pl.BlockSpec(memory_space=pl.ANY)
    return pl.pallas_call(
        kernel,
        out_shape=(jax.ShapeDtypeStruct((XD, PIECE, 128), BF), jax.ShapeDtypeStruct((2 * XD, 1, 128), F32)),
        in_specs=[pl.BlockSpec(memory_space=pltpu.SMEM)] + [any_] * 5,
        out_specs=(any_, any_),
        scratch_shapes=scratch,
        name="prefix_attention",
        compiler_params=pltpu.CompilerParams(collective_id=0, has_side_effects=True, vmem_limit_bytes=63 << 20),
    )


def make_finish(tok):
    rows = RATIO * tok

    def kernel(o_in, l_in, o_out, l_out, o_buf, l_buf, table, sem):
        o_get = pltpu.make_async_copy(o_in, o_buf, sem.at[0])
        l_get = pltpu.make_async_copy(l_in, l_buf, sem.at[1])
        o_get.start()
        l_get.start()
        l_get.wait()
        lane = lax.broadcasted_iota(jnp.int32, (1, 128), 1)
        head_rows = []
        for i in range(KV):
            pair = l_buf[pl.ds(2 * i, 2)].reshape(2, 128)
            for g in range(RATIO):
                s = g * tok
                lo, back = pair[s // 128:s // 128 + 1], 128 - s % 128
                head_rows.append(lo if back == 128 else jnp.where(
                    lane < back, pltpu.roll(lo, back, 1), pltpu.roll(pair[1:2], back, 1)))
        table[...] = jnp.concatenate(head_rows + [jnp.zeros((32 - HEADS, 128), F32)], axis=0).T[:tok, :HEADS]
        l_put = pltpu.make_async_copy(table, l_out, sem.at[2])
        l_put.start()
        o_get.wait()
        o_put = pltpu.make_async_copy(o_buf, o_out, sem.at[3])
        o_put.start()
        l_put.wait()
        o_put.wait()

    V, any_ = pltpu.VMEM, pl.BlockSpec(memory_space=pl.ANY)
    return pl.pallas_call(
        kernel,
        out_shape=(jax.ShapeDtypeStruct((KV, rows, HD), BF), jax.ShapeDtypeStruct((tok, HEADS), F32)),
        in_specs=[any_, any_],
        out_specs=(any_, any_),
        scratch_shapes=[V((KV, rows, HD), BF), V((2 * KV, 1, 128), F32), V((tok, HEADS), F32),
                        pltpu.SemaphoreType.DMA((4,))],
        name="final_form",
    )


def solution(mesh):
    spec = P(("dp", "cp"))

    def local(queries, key_new, value_new, key_cache, value_cache, prefix_len):
        tok, cache = queries.shape[0], key_cache.shape[0]
        call = make_kernel(tok, cache)
        q = queries.transpose(1, 0, 2).reshape(KV, RATIO * tok, HD)

        def rows(a):
            return a.reshape(a.shape[0] * KV, HD)

        out, row_lse = make_finish(tok)(*call(prefix_len, q, rows(key_cache), rows(value_cache), rows(key_new), rows(value_new)))
        return out.reshape(HEADS, tok, HD).transpose(1, 0, 2), row_lse

    return jax.shard_map(local, mesh=mesh, in_specs=(spec,) * 5 + (P("dp"),), out_specs=(spec, spec), check_vma=False)
```
